256 devices in a mesh: seq: 64 (over x, y, z_lo), rep: 4 (over z_hi, core).
Axes of the slice: x: 4, y: 4, z: 8 (z_hi: 2, z_lo: 4; z = z_hi * 4 + z_lo), core: 2. Of those that a mesh axis runs over, the one named last changes fastest.
Arguments:
- prefix_cache: bfloat16 [2, 2, 1024, 32768], P(None, None, 'seq', 'rep'), may hold values from -5 to 5
- queries: bfloat16 [2, 256, 4096], P(None, ('seq', 'rep')), may hold values from -12 to 12
- suffix_cache: bfloat16 [2, 256, 2, 128, 1024], P(None, ('seq', 'rep')), may hold values from -9 to 9
- suffix_lengths: int32 [256], replicated, may hold values from 1 to 128, as said below
- slot_request: int32 [256], P(('seq', 'rep')), may hold values from 0 to 255, each once
Outputs:
- attended: bfloat16 [2, 256, 4096], P(None, ('seq', 'rep'))
The draws below stay inside these ranges and needn't reach their ends.
Inputs may be any that keep to these rules, and one draw needn't show every extreme that they name: `suffix_lengths`: every request has 1 to 128 suffix tokens; some request has exactly 128. `slot_request`: every request id stands in exactly one slot.
All inputs are finite; a program needn't handle non-finite values.
Results may differ from the reference program's by a relative error of at most 0.005.
Values may be sent and summed in bfloat16 or wider, within the bound.
A program may use at most 64 MiB of HBM per device.

```python
import jax
import jax.numpy as jnp
from jax import lax

QH = 32
KVH = 8
HD = 128
LAYERS = 2
SUF = 128
GROUP = 4
KV_FEAT = 1024
PREFIX = 32768
REQUESTS = 256


def draw_prefix_cache(key, part):
    fresh_key = jax.random.fold_in(key, 11)
    shape_full = (LAYERS, 2, KVH * HD, PREFIX)
    drawn = jnp.clip(jax.random.normal(fresh_key, shape_full, jnp.float32), -5.0, 5.0)
    return drawn.astype(jnp.bfloat16)


def draw_queries(key, part):
    fresh_key = jax.random.fold_in(key, 13)
    shape_full = (LAYERS, REQUESTS, QH * HD)
    drawn = jnp.clip(3.0 * jax.random.normal(fresh_key, shape_full, jnp.float32), -12.0, 12.0)
    return drawn.astype(jnp.bfloat16)


def draw_suffix_lengths(key, part):
    length_key, top_key = jax.random.split(jax.random.fold_in(key, 23))
    drawn = jax.random.randint(length_key, (REQUESTS,), 1, SUF + 1)
    top_index = jax.random.randint(top_key, (), 0, REQUESTS)
    return jnp.where(jnp.arange(REQUESTS) == top_index, SUF, drawn).astype(jnp.int32)


def level_of(stream_key, extent, cuts, smallest, high):
    def one(position, shards_of):
        steps = jax.random.uniform(jax.random.fold_in(jax.random.fold_in(stream_key, 6), position), (shards_of,), jnp.float32, smallest / len(cuts), high / len(cuts))
        return jnp.repeat(jnp.exp(steps), extent[position] // shards_of).reshape((-1,) + (1,) * (len(extent) - position - 1))

    factor_of = one(*cuts[0])
    for cut in cuts[1:]:
        factor_of = factor_of * one(*cut)
    return factor_of


def gaussian(stream_key, extent, scale, limit, cuts=(), held_as=jnp.bfloat16):
    array = scale * jax.random.normal(stream_key, extent, jnp.float32)
    if cuts:
        array = array * level_of(stream_key, extent, cuts, -0.22, 0.18)
    return jnp.clip(array, -limit, limit).astype(held_as)


def setup_inputs(seed: int = 0) -> dict:
    keys = jax.random.split(jax.random.key(seed), 6)
    return {
        "prefix_cache": draw_prefix_cache(jax.random.fold_in(keys[5], 71), 0),
        "queries": draw_queries(jax.random.fold_in(keys[5], 71), 0),
        "suffix_cache": gaussian(keys[2], (LAYERS, REQUESTS, 2, SUF, KV_FEAT), 1.5, 9.0, ((1, 256),)),
        "suffix_lengths": draw_suffix_lengths(jax.random.fold_in(keys[5], 71), 0),
        "slot_request": jax.random.permutation(keys[4], REQUESTS).astype(jnp.int32),
    }


neg_fill = -1.0e30
block_rows = 8


def attend(query_rows, key_block, value_block, suffix_rows, length_rows):
    row_count = query_rows.shape[0]
    score_scale = HD ** -0.5
    shaped = query_rows.astype(jnp.float32).reshape(row_count, KVH, GROUP, HD)
    scores = jnp.einsum("rhgd,hdp->rhgp", shaped, key_block, precision=lax.Precision.HIGHEST) * score_scale
    prefix_top = jnp.max(scores, axis=3)
    weights = jnp.exp(scores - prefix_top[..., None]).astype(jnp.bfloat16)
    weights = lax.optimization_barrier(weights).astype(jnp.float32)
    prefix_den = jnp.sum(weights, axis=3)
    prefix_num = jnp.einsum("rhgp,hdp->rhgd", weights, value_block, precision=lax.Precision.HIGHEST)
    suffix_keys = suffix_rows[:, 0].astype(jnp.float32).reshape(row_count, SUF, KVH, HD)
    suffix_values = suffix_rows[:, 1].astype(jnp.float32).reshape(row_count, SUF, KVH, HD)
    suffix_scores = jnp.einsum("rhgd,rshd->rhgs", shaped, suffix_keys, precision=lax.Precision.HIGHEST) * score_scale
    valid_mask = (jnp.arange(SUF, dtype=jnp.int32)[None, :] < length_rows[:, None])[:, None, None, :]
    suffix_scores = jnp.where(valid_mask, suffix_scores, neg_fill)
    suffix_top = jnp.max(suffix_scores, axis=3)
    suffix_weights = jnp.where(valid_mask, jnp.exp(suffix_scores - suffix_top[..., None]), 0.0).astype(jnp.bfloat16)
    suffix_weights = lax.optimization_barrier(suffix_weights).astype(jnp.float32)
    suffix_den = jnp.sum(suffix_weights, axis=3)
    suffix_num = jnp.einsum("rhgs,rshd->rhgd", suffix_weights, suffix_values, precision=lax.Precision.HIGHEST)
    both_top = jnp.maximum(prefix_top, suffix_top)
    prefix_scale = jnp.exp(prefix_top - both_top)
    suffix_scale = jnp.exp(suffix_top - both_top)
    total_den = prefix_scale * prefix_den + suffix_scale * suffix_den
    mixed = (prefix_scale[..., None] * prefix_num + suffix_scale[..., None] * suffix_num) / total_den[..., None]
    return mixed.reshape(row_count, QH * HD).astype(jnp.bfloat16)


def reference(prefix_cache, queries, suffix_cache, suffix_lengths, slot_request):
    lengths = suffix_lengths[slot_request]
    blocks = REQUESTS // block_rows
    results = []
    for layer_index in range(LAYERS):
        key_block = prefix_cache[layer_index, 0].astype(jnp.float32).reshape(KVH, HD, PREFIX)
        value_block = prefix_cache[layer_index, 1].astype(jnp.float32).reshape(KVH, HD, PREFIX)
        query_rows = queries[layer_index].reshape(blocks, block_rows, QH * HD)
        suffix_rows = suffix_cache[layer_index].reshape(blocks, block_rows, 2, SUF, KVH * HD)
        length_rows = lengths.reshape(blocks, block_rows)

        def one_block(packed):
            return attend(packed[0], key_block, value_block, packed[1], packed[2])

        attended = lax.map(one_block, (query_rows, suffix_rows, length_rows))
        results.append(attended.reshape(REQUESTS, QH * HD))
    return jnp.stack(results)
```

```python
import functools
import math

import jax
import jax.numpy as jnp
from jax import lax
from jax.experimental import pallas as pl
from jax.experimental.pallas import tpu as pltpu
from jax.sharding import PartitionSpec as P

QH = 32
KVH = 8
HD = 128
SUF = 128
GROUP = 4
NEG = -1e30
SCALE2 = HD ** -0.5 * math.log2(math.e)
POS = 1024
NT = (((1,), (1,)), ((), ()))
NN = (((1,), (0,)), ((), ()))
MESH = pl.DeviceIdType.MESH


def dot(a, b, dims):
    return lax.dot_general(a, b, dims, preferred_element_type=jnp.float32)


def kernel(
    prefix, qmsg, suffix, lengths, slot, out,
    stage, kown, koth, suf, qa, qall, wbuf, lrep, rden, sbuf_o, sbuf_l,
    osend, lsend, orecv, lrecv, fsend, frecv,
    loc_sem, a_s, a_r, kv_s, kv_r, b_s, b_r, y_sem, f_s, f_r, c_s, c_r, l_s, l_r, d_s, d_r,
):
    seq = lax.axis_index("seq")
    rep = lax.axis_index("rep")
    x, y, zl = seq // 16, (seq // 4) % 4, seq % 4
    yh, yl = y // 2, y % 2
    zh, c = rep // 2, rep % 2
    z = zh * 4 + zl
    head = x * 2 + yh
    part = yl * 4 + zl
    place = yl * 8 + z

    def at(head_to, yl_to, z_to, c_to):
        x_to, yh_to = head_to // 2, head_to % 2
        return ((x_to * 4 + yh_to * 2 + yl_to) * 4 + z_to % 4, (z_to // 4) * 2 + c_to)

    def remote(src, dst, s, r, dev):
        return pltpu.make_async_remote_copy(
            src_ref=src, dst_ref=dst, send_sem=s, recv_sem=r, device_id=dev, device_id_type=MESH)

    loads = [pltpu.make_async_copy(prefix.at[l, k], stage.at[l, k], loc_sem.at[l * 2 + k])
             for l in range(2) for k in range(2)]
    owns = [pltpu.make_async_copy(
        prefix.at[l, k, :, pl.ds(pl.multiple_of(part * POS, POS), POS)],
        kown.at[l, k, part], loc_sem.at[4 + l * 2 + k]) for l in range(2) for k in range(2)]
    load_suf = pltpu.make_async_copy(suffix, suf, loc_sem.at[8])
    for cp in loads + owns:
        cp.start()
    load_suf.start()

    barrier = pltpu.get_barrier_semaphore()
    peers = []
    for k in range(1, 8):
        peers.append(at((head + k) % 8, yl, z, c))
    for k in range(1, 16):
        to = (place + k) % 16
        peers.append(at(head, to // 8, to % 8, c))
    other = at(head, yl, z, 1 - c)
    peers.append(other)
    for dev in peers:
        pl.semaphore_signal(barrier, inc=1, device_id=dev, device_id_type=MESH)
    pl.semaphore_wait(barrier, len(peers))

    def a_copy(k):
        to = (head + k) % 8
        return remote(qmsg.at[to], qa.at[head], a_s.at[k], a_r.at[head], at(to, yl, z, c))

    for k in range(1, 8):
        a_copy(k).start()
    qa[head] = qmsg[head]

    steps = [(2, 0), (2, 1), (1, 0), (1, 1), (3, 0), (3, 1), (0, 1)]

    def kv_copy(l, k, i):
        dz, dy = steps[i]
        yl_to, zl_to = (yl + dy) % 2, (zl + dz) % 4
        to = yl_to * 4 + zl_to
        return remote(
            stage.at[l, k, :, pl.ds(pl.multiple_of(to * POS, POS), POS)],
            kown.at[l, k, part], kv_s.at[l * 2 + k, i], kv_r.at[l * 2 + k, part],
            at(head, yl_to, zh * 4 + zl_to, c))

    def kv_send(l, k):
        loads[l * 2 + k].wait()
        for i in range(7):
            kv_copy(l, k, i).start()

    def kv_wait(l, k):
        owns[l * 2 + k].wait()
        for i in range(1, 8):
            src = (part + i) % 8
            remote(kown.at[l, k, src], kown.at[l, k, src], kv_s.at[l * 2 + k, 0],
                   kv_r.at[l * 2 + k, src], other).wait_recv()

    def forward(l, k):
        return remote(kown.at[l, k], koth.at[l, k], f_s.at[l * 2 + k], f_r.at[l * 2 + k], other)

    kv_send(0, 0)

    for k in range(1, 8):
        src = (head + k) % 8
        remote(qa.at[src], qa.at[src], a_s.at[0], a_r.at[src], other).wait_recv()
    mine = jnp.swapaxes(qa[...].astype(jnp.float32), 0, 1).reshape(64, HD)
    qall[place] = mine.astype(jnp.bfloat16)

    def b_copy(k):
        return remote(qall.at[place], qall.at[place], b_s.at[k], b_r.at[z],
                      at(head, yl, (z + k) % 8, c))

    load_suf.wait()
    count = lengths[slot[0]]
    row = lax.broadcasted_iota(jnp.int32, (8, HD), 0)
    lane = lax.broadcasted_iota(jnp.int32, (8, HD), 1)
    valid = lane < count

    def suffix_head(h):
        cols = slice(h * HD, (h + 1) * HD)
        q = qmsg[h]
        s0 = dot(q, suf[0, 0, 0, :, cols], NT)
        s1 = dot(q, suf[1, 0, 0, :, cols], NT)
        s = jnp.where(valid, jnp.where(row < GROUP, s0, s1) * SCALE2, NEG)
        top = jnp.max(s, axis=1, keepdims=True)
        w = jnp.where(valid, jnp.exp2(s - top), 0.0).astype(jnp.bfloat16)
        den = jnp.sum(w.astype(jnp.float32), axis=1, keepdims=True)
        n0 = dot(w, suf[0, 0, 1, :, cols], NN)
        n1 = dot(w, suf[1, 0, 1, :, cols], NN)
        sbuf_o[h] = jnp.where(row < GROUP, n0, n1) / den
        sbuf_l[h] = jnp.broadcast_to(top + jnp.log2(den), (8, HD))

    suffix_head(0)
    for k in (4, 3, 5, 2, 6, 1, 7):
        b_copy(k).start()
    kv_send(0, 1)
    kv_send(1, 0)
    kv_send(1, 1)
    for h in range(1, KVH):
        suffix_head(h)

    for k in range(1, 8):
        src = yl * 8 + (z + k) % 8
        remote(qall.at[src], qall.at[src], b_s.at[0], b_r.at[(z + k) % 8], other).wait_recv()
    half = pl.ds(yl * 8, 8)
    rest = pl.ds((1 - yl) * 8, 8)
    y_copy = remote(qall.at[half], qall.at[half], y_sem.at[0], y_sem.at[1], at(head, 1 - yl, z, c))
    y_copy.start()
    kv_wait(0, 0)
    forward(0, 0).start()
    remote(qall.at[rest], qall.at[rest], y_sem.at[0], y_sem.at[1], other).wait_recv()

    def weights(l):
        remote(koth.at[l, 0], koth.at[l, 0], f_s.at[l * 2], f_r.at[l * 2], other).wait_recv()

        def rows(i, carry):
            q = qall[pl.ds(i * 4, 4), l * 32:(l + 1) * 32, :].reshape(128, HD)
            at_rows = pl.ds(pl.multiple_of(i * 128, 128), 128)
            sa = dot(q, kown[l, 0].reshape(HD, POS), NN) * SCALE2
            sb = dot(q, koth[l, 0].reshape(HD, POS), NN) * SCALE2
            top = jnp.maximum(jnp.max(sa, axis=1, keepdims=True), jnp.max(sb, axis=1, keepdims=True))
            wa = jnp.exp2(sa - top).astype(jnp.bfloat16)
            wb = jnp.exp2(sb - top).astype(jnp.bfloat16)
            den = jnp.sum(wa.astype(jnp.float32) + wb.astype(jnp.float32), axis=1, keepdims=True)
            wbuf[0, at_rows, :] = wa
            wbuf[1, at_rows, :] = wb
            lrep[at_rows, :] = jnp.broadcast_to(top + jnp.log2(den), (128, HD))
            rden[at_rows, :] = jnp.broadcast_to(1.0 / den, (128, HD))
            return carry

        lax.fori_loop(0, 4, rows, 0)

    def values(l):
        row32 = lax.broadcasted_iota(jnp.int32, (4, 32, HD), 1)
        lane32 = lax.broadcasted_iota(jnp.int32, (4, 32, HD), 2)

        remote(koth.at[l, 1], koth.at[l, 1], f_s.at[l * 2 + 1], f_r.at[l * 2 + 1], other).wait_recv()

        def rows(i, carry):
            at_rows = pl.ds(pl.multiple_of(i * 128, 128), 128)
            o = dot(wbuf[0, at_rows, :], kown[l, 1].reshape(HD, POS), NT)
            o = o + dot(wbuf[1, at_rows, :], koth[l, 1].reshape(HD, POS), NT)
            o = o * rden[at_rows, :]
            osend[l, pl.ds(i * 4, 4)] = o.astype(jnp.bfloat16).reshape(4, 32, HD)
            lx = lrep[at_rows, :].reshape(4, 32, HD)
            lsend[l, pl.ds(i * 4, 4)] = jnp.sum(
                jnp.where(row32 == lane32, lx, 0.0), axis=1, keepdims=True)
            return carry

        lax.fori_loop(0, 4, rows, 0)
        for k in range(1, 16):
            to = (place + k) % 16
            dev = at(head, to // 8, to % 8, c)
            remote(osend.at[l, to], orecv.at[l, place], c_s.at[l, k], c_r.at[l, place], dev).start()
            remote(lsend.at[l, to], lrecv.at[l, place], l_s.at[l, k], l_r.at[l, place], dev).start()
        orecv[l, place] = osend[l, place]
        lrecv[l, place] = lsend[l, place]

    weights(0)
    kv_wait(0, 1)
    forward(0, 1).start()
    values(0)
    kv_wait(1, 0)
    forward(1, 0).start()
    weights(1)
    kv_wait(1, 1)
    forward(1, 1).start()
    values(1)

    def combine(l):
        for k in range(1, 16):
            src = (place + k) % 16
            remote(orecv.at[l, src], orecv.at[l, src], c_s.at[l, 0], c_r.at[l, src], other).wait_recv()
            remote(lrecv.at[l, src], lrecv.at[l, src], l_s.at[l, 0], l_r.at[l, src], other).wait_recv()
        ls = lrecv[l].reshape(16, HD)
        top = jnp.max(ls, axis=0, keepdims=True)
        w = jnp.exp2(ls - top)
        den = jnp.sum(w, axis=0, keepdims=True)
        w = w / den
        total = jnp.broadcast_to(top + jnp.log2(den), (112, HD))
        cols = jnp.concatenate([w, total], axis=0).T
        o = jnp.zeros((32, HD), jnp.float32)
        for s in range(16):
            o = o + orecv[l, s].astype(jnp.float32) * cols[:32, s:s + 1]
        lall = jnp.broadcast_to(cols[:32, 16:17], (32, HD))
        both = jnp.concatenate([o.reshape(4, 8, HD), lall.reshape(4, 8, HD)], axis=0)
        fsend[l] = jnp.swapaxes(both, 0, 1)
        for k in range(1, 8):
            to = (head + k) % 8
            remote(fsend.at[l, to], frecv.at[l, head], d_s.at[l, k], d_r.at[l, head],
                   at(to, yl, z, c)).start()
        frecv[l, head] = fsend[l, head]

    def finish(l):
        for k in range(1, 8):
            src = (head + k) % 8
            remote(frecv.at[l, src], frecv.at[l, src], d_s.at[l, 0], d_r.at[l, src], other).wait_recv()
        got = frecv[l]
        o_p, l_p = got[:, :GROUP, :], got[:, GROUP:, :]
        o_s = sbuf_o[...][:, l * GROUP:(l + 1) * GROUP, :]
        l_s_ = sbuf_l[...][:, l * GROUP:(l + 1) * GROUP, :]
        top = jnp.maximum(l_p, l_s_)
        a = jnp.exp2(l_p - top)
        b = jnp.exp2(l_s_ - top)
        out[l] = ((a * o_p + b * o_s) / (a + b)).astype(jnp.bfloat16)

    combine(0)
    combine(1)
    finish(0)
    finish(1)

    for k in range(1, 8):
        a_copy(k).wait_send()
        b_copy(k).wait_send()
    y_copy.wait_send()
    for l in range(2):
        for k in range(2):
            for i in range(7):
                kv_copy(l, k, i).wait_send()
            forward(l, k).wait_send()
        for k in range(1, 16):
            remote(osend.at[l, 0], orecv.at[l, 0], c_s.at[l, k], c_r.at[l, 0], other).wait_send()
            remote(lsend.at[l, 0], lrecv.at[l, 0], l_s.at[l, k], l_r.at[l, 0], other).wait_send()
        for k in range(1, 8):
            remote(fsend.at[l, 0], frecv.at[l, 0], d_s.at[l, k], d_r.at[l, 0], other).wait_send()


def body(prefix_cache, queries, suffix_cache, suffix_lengths, slot_request):
    bf, f32 = jnp.bfloat16, jnp.float32
    qmsg = queries.reshape(2, KVH, GROUP, HD).transpose(1, 0, 2, 3).reshape(KVH, 2 * GROUP, HD)
    dma = pltpu.SemaphoreType.DMA
    any_space = pl.BlockSpec(memory_space=pl.ANY)
    out = pl.pallas_call(
        kernel,
        out_shape=jax.ShapeDtypeStruct((2, KVH, GROUP, HD), bf),
        in_specs=[
            any_space,
            pl.BlockSpec(memory_space=pltpu.VMEM),
            any_space,
            pl.BlockSpec(memory_space=pltpu.SMEM),
            pl.BlockSpec(memory_space=pltpu.SMEM),
        ],
        out_specs=pl.BlockSpec(memory_space=pltpu.VMEM),
        scratch_shapes=[
            pltpu.VMEM((2, 2, 16, 8192), bf),
            pltpu.VMEM((2, 2, 8, 16, POS), bf),
            pltpu.VMEM((2, 2, 8, 16, POS), bf),
            pltpu.VMEM((2, 1, 2, SUF, KVH * HD), bf),
            pltpu.VMEM((8, 8, HD), bf),
            pltpu.VMEM((16, 64, HD), bf),
            pltpu.VMEM((2, 512, POS), bf),
            pltpu.VMEM((512, HD), f32),
            pltpu.VMEM((512, HD), f32),
            pltpu.VMEM((KVH, 8, HD), f32),
            pltpu.VMEM((KVH, 8, HD), f32),
            pltpu.VMEM((2, 16, 32, HD), bf),
            pltpu.VMEM((2, 16, 1, HD), f32),
            pltpu.VMEM((2, 16, 32, HD), bf),
            pltpu.VMEM((2, 16, 1, HD), f32),
            pltpu.VMEM((2, 8, 8, HD), f32),
            pltpu.VMEM((2, 8, 8, HD), f32),
            dma((9,)),
            dma((8,)), dma((8,)),
            dma((4, 8)), dma((4, 8)),
            dma((8,)), dma((8,)),
            dma((2,)),
            dma((4,)), dma((4,)),
            dma((2, 16)), dma((2, 16)),
            dma((2, 16)), dma((2, 16)),
            dma((2, 8)), dma((2, 8)),
        ],
        compiler_params=pltpu.CompilerParams(collective_id=0, has_side_effects=True),
        name="attend",
    )(prefix_cache, qmsg, suffix_cache, suffix_lengths, slot_request)
    return out.reshape(2, 1, QH * HD)


def solution(mesh):
    in_specs = (
        P(None, None, "seq", "rep"),
        P(None, ("seq", "rep"), None),
        P(None, ("seq", "rep"), None, None, None),
        P(),
        P(("seq", "rep")),
    )
    out_specs = P(None, ("seq", "rep"), None)
    return jax.shard_map(body, mesh=mesh, in_specs=in_specs, out_specs=out_specs, check_vma=False)
```

```python
import math

import jax
import jax.numpy as jnp
from jax import lax
from jax.experimental import pallas as pl
from jax.experimental.pallas import tpu as pltpu
from jax.sharding import PartitionSpec as P

QH = 32
KVH = 8
HD = 128
SUF = 128
GROUP = 4
NEG = -1e30
SCALE2 = HD ** -0.5 * math.log2(math.e)
POS = 1024
NT = (((1,), (1,)), ((), ()))
NN = (((1,), (0,)), ((), ()))
MESH = pl.DeviceIdType.MESH


def dot(a, b, dims):
    return lax.dot_general(a, b, dims, preferred_element_type=jnp.float32)


def kernel(
    prefix, queries, suffix, lengths, slot, out,
    stage, kown, koth, suf, qraw, qmsg, qa, qall, wbuf, rden, oacc, sbuf_o, sbuf_l,
    osend, orecv, lsend, lrecv, gsend, grecv, fsend, frecv,
    loc_sem, a_sem, b_sem, y_sem, kv_s, kv_r, v1_r, f_s, f_r, c_s, c_r, l_sem, g_sem, d_s, d_r,
):
    f32, bf16 = jnp.float32, jnp.bfloat16
    seq = lax.axis_index("seq")
    rep = lax.axis_index("rep")
    x, y, zl = seq // 16, (seq // 4) % 4, seq % 4
    yh, yl = y // 2, y % 2
    zh, c = rep // 2, rep % 2
    z = zh * 4 + zl
    head = x * 2 + yh
    part = yl * 4 + zl
    spot = head * 2 + yl

    def at(head_to, yl_to, z_to, c_to):
        x_to, yh_to = head_to // 2, head_to % 2
        return ((x_to * 4 + yh_to * 2 + yl_to) * 4 + z_to % 4, (z_to // 4) * 2 + c_to)

    other = at(head, yl, z, 1 - c)

    def remote(src, dst, s, r, dev=other):
        return pltpu.make_async_remote_copy(
            src_ref=src, dst_ref=dst, send_sem=s, recv_sem=r, device_id=dev, device_id_type=MESH)

    load_q = pltpu.make_async_copy(queries, qraw, loc_sem.at[9])
    load_q.start()
    order = ((0, 0), (1, 0), (0, 1), (1, 1))
    loads = {(l, k): pltpu.make_async_copy(prefix.at[l, k], stage.at[l, k], loc_sem.at[l * 2 + k])
             for l, k in order}
    owns = {(l, k): pltpu.make_async_copy(
        prefix.at[l, k, :, pl.ds(pl.multiple_of(part * POS, POS), POS)],
        kown.at[l, k, part], loc_sem.at[4 + l * 2 + k]) for l, k in order}
    load_suf = pltpu.make_async_copy(suffix, suf, loc_sem.at[8])
    loads[0, 0].start()
    load_suf.start()

    barrier = pltpu.get_barrier_semaphore()
    peers = [other]
    for k in range(1, 16):
        to = (spot + k) % 16
        peers.append(at(to // 2, to % 2, z, c))
    for k in range(1, 8):
        peers.append(at(head, yl, (z + k) % 8, c))
    for k in range(1, 4):
        peers.append(at(head, 1 - yl, zh * 4 + (zl + k) % 4, c))
    for dev in peers:
        pl.semaphore_signal(barrier, inc=1, device_id=dev, device_id_type=MESH)
    for l, k in order:
        if (l, k) != (0, 0):
            loads[l, k].start()
        owns[l, k].start()

    load_q.wait()
    q32 = qraw[...].astype(f32)
    for h in range(KVH):
        rows = [q32[l:l + 1, (h * GROUP + g) * HD:(h * GROUP + g + 1) * HD]
                for l in range(2) for g in range(GROUP)]
        qmsg[h] = jnp.concatenate(rows, axis=0).astype(bf16)
    loads[0, 0].wait()
    pl.semaphore_wait(barrier, len(peers))

    for k in range(1, 8):
        to = (head + k) % 8
        remote(qmsg.at[to], qa.at[head], a_sem.at[0], a_sem.at[1], at(to, yl, z, c)).start()
    qa[head] = qmsg[head]

    def kv_send(l, k, steps):
        for dz, dy in steps:
            yl_to, zl_to = (yl + dy) % 2, (zl + dz) % 4
            to = yl_to * 4 + zl_to
            remote(
                stage.at[l, k, :, pl.ds(pl.multiple_of(to * POS, POS), POS)],
                kown.at[l, k, part], kv_s.at[l * 2 + k],
                v1_r.at[part] if (l, k) == (1, 1) else kv_r.at[l * 2 + k],
                at(head, yl_to, zh * 4 + zl_to, c)).start()

    def kv_wait(l, k):
        owns[l, k].wait()
        remote(kown.at[l, k, 0:7], kown.at[l, k, 0:7], kv_s.at[0], kv_r.at[l * 2 + k]).wait_recv()

    def forward(l, k):
        return remote(kown.at[l, k], koth.at[l, k], f_s.at[l * 2 + k], f_r.at[l * 2 + k])

    early = [(2, 0), (2, 1), (0, 1), (1, 0)]
    late = [(1, 1), (3, 0), (3, 1)]
    full = [(2, 0), (2, 1), (1, 0), (1, 1), (3, 0), (3, 1), (0, 1)]

    kv_send(0, 0, early)

    load_suf.wait()
    count = lengths[slot[0]]
    row = lax.broadcasted_iota(jnp.int32, (8, HD), 0)
    lane = lax.broadcasted_iota(jnp.int32, (8, HD), 1)
    valid = lane < count

    def suffix_head(h):
        cols = slice(h * HD, (h + 1) * HD)
        q = qmsg[h]
        s0 = dot(q, suf[0, 0, 0, :, cols], NT)
        s1 = dot(q, suf[1, 0, 0, :, cols], NT)
        s = jnp.where(valid, jnp.where(row < GROUP, s0, s1) * SCALE2, NEG)
        top = jnp.max(s, axis=1, keepdims=True)
        w = jnp.where(valid, jnp.exp2(s - top), 0.0).astype(bf16)
        den = jnp.sum(w.astype(f32), axis=1, keepdims=True)
        n0 = dot(w, suf[0, 0, 1, :, cols], NN)
        n1 = dot(w, suf[1, 0, 1, :, cols], NN)
        sbuf_o[h] = jnp.where(row < GROUP, n0, n1) / den
        sbuf_l[h] = jnp.broadcast_to(top + jnp.log2(den), (8, HD))

    def suffix_part():
        for h in range(KVH):
            suffix_head(h)

    suffix_part()

    def a_wait():
        remote(qa.at[0:7], qa.at[0:7], a_sem.at[0], a_sem.at[1]).wait_recv()

    a_wait()
    qall[z, yl] = jnp.swapaxes(qa[...].astype(f32), 0, 1).reshape(64, HD).astype(bf16)
    loads[1, 0].wait()
    for k in (4, 3, 5, 2, 6, 1, 7):
        remote(qall.at[z, yl], qall.at[z, yl], b_sem.at[0], b_sem.at[1],
               at(head, yl, (z + k) % 8, c)).start()
    kv_send(0, 0, late)
    kv_send(1, 0, full)
    loads[0, 1].wait()
    loads[1, 1].wait()

    def b_wait():
        remote(qall.at[0:7, 0], qall.at[0:7, 0], b_sem.at[0], b_sem.at[1]).wait_recv()

    def y_copy(which):
        return remote(qall.at[:, which], qall.at[:, which], y_sem.at[0], y_sem.at[1],
                      at(head, 1 - yl, z, c))

    def y_wait():
        y_copy(1 - yl).wait_recv()

    b_wait()
    y_copy(yl).start()
    kv_send(0, 1, full)
    kv_send(1, 1, full)

    def weights(l):
        forward(l, 0).wait_recv()
        r64 = lax.broadcasted_iota(jnp.int32, (2, 64, HD), 1)
        c64 = lax.broadcasted_iota(jnp.int32, (2, 64, HD), 2)

        def rows(i, carry):
            q = qall[pl.ds(i * 2, 2), :, l * 32:(l + 1) * 32, :].reshape(128, HD)
            at_rows = pl.ds(pl.multiple_of(i * 128, 128), 128)
            sa = dot(q, kown[l, 0].reshape(HD, POS), NN) * SCALE2
            sb = dot(q, koth[l, 0].reshape(HD, POS), NN) * SCALE2
            top = jnp.maximum(jnp.max(sa, axis=1, keepdims=True), jnp.max(sb, axis=1, keepdims=True))
            wa = jnp.exp2(sa - top).astype(bf16)
            wb = jnp.exp2(sb - top).astype(bf16)
            den = jnp.sum(wa.astype(f32) + wb.astype(f32), axis=1, keepdims=True)
            wbuf[l, 0, at_rows, :] = wa
            wbuf[l, 1, at_rows, :] = wb
            rden[l, at_rows, :] = jnp.broadcast_to(1.0 / den, (128, HD))
            big = jnp.broadcast_to(top + jnp.log2(den), (128, HD)).reshape(2, 64, HD)
            line = jnp.sum(jnp.where(c64 == r64 + l * 64, big, 0.0), axis=1, keepdims=True)
            if l == 0:
                lsend[pl.ds(i * 2, 2)] = line
            else:
                lsend[pl.ds(i * 2, 2)] = lsend[pl.ds(i * 2, 2)] + line
            return carry

        lax.fori_loop(0, 4, rows, 0)

    def values_own(l):
        def rows(i, carry):
            at_rows = pl.ds(pl.multiple_of(i * 128, 128), 128)
            oacc[at_rows, :] = dot(wbuf[l, 0, at_rows, :], kown[l, 1].reshape(HD, POS), NT)
            return carry

        lax.fori_loop(0, 4, rows, 0)

    def values_other(l):
        forward(l, 1).wait_recv()
        for i in range(4):
            at_rows = slice(i * 128, (i + 1) * 128)
            o = oacc[at_rows, :] + dot(wbuf[l, 1, at_rows, :], koth[l, 1].reshape(HD, POS), NT)
            o = o * rden[l, at_rows, :]
            osend[l, 2 * i:2 * i + 2] = o.astype(bf16).reshape(2, 64, HD)
            for to in (2 * i, 2 * i + 1):
                @pl.when(z != to)
                def _():
                    remote(osend.at[l, to], orecv.at[l, z], c_s.at[l], c_r.at[l],
                           at(head, yl, to, c)).start()
        orecv[l, z] = osend[l, z]

    kv_wait(0, 0)
    forward(0, 0).start()
    y_wait()
    weights(0)
    kv_wait(1, 0)
    forward(1, 0).start()
    weights(1)
    for k in range(1, 8):
        to = (z + k) % 8
        remote(lsend.at[to], lrecv.at[z], l_sem.at[0], l_sem.at[1], at(head, yl, to, c)).start()
    lrecv[z] = lsend[z]
    kv_wait(0, 1)
    forward(0, 1).start()
    values_own(0)
    values_other(0)

    def last_pieces():
        owns[1, 1].wait()
        remote(kown.at[1, 1, part], koth.at[1, 1, part], f_s.at[3], f_r.at[3]).start()
        for dz, dy in full:
            src = (yl + dy) % 2 * 4 + (zl + 4 - dz) % 4
            piece = kown.at[1, 1, src]
            remote(piece, piece, kv_s.at[0], v1_r.at[src]).wait_recv()
            remote(piece, koth.at[1, 1, src], f_s.at[3], f_r.at[3]).start()

    last_pieces()
    values_own(1)
    values_other(1)

    def sources():
        remote(lrecv.at[0:7], lrecv.at[0:7], l_sem.at[0], l_sem.at[1]).wait_recv()
        ls = lrecv[...].reshape(8, HD)
        top = jnp.max(ls, axis=0, keepdims=True)
        w = jnp.exp2(ls - top)
        den = jnp.sum(w, axis=0, keepdims=True)
        total = jnp.broadcast_to(top + jnp.log2(den), (120, HD))
        cols = jnp.concatenate([w / den, total], axis=0).T
        big = jnp.broadcast_to(cols[:, 8:9], (128, HD)).reshape(2, 2, GROUP, 8, HD)
        both = [jnp.swapaxes(big[:, to].reshape(8, 8, HD), 0, 1) for to in range(2)]
        gsend[...] = jnp.stack(both, axis=1).reshape(16, 8, HD)
        for k in range(1, 16):
            to = (spot + k) % 16
            remote(gsend.at[to], grecv.at[spot], g_sem.at[0], g_sem.at[1],
                   at(to // 2, to % 2, z, c)).start()
        grecv[spot] = gsend[spot]
        return cols

    def combine(l, cols):
        remote(orecv.at[l, 0:7], orecv.at[l, 0:7], c_s.at[l], c_r.at[l]).wait_recv()
        o = jnp.zeros((64, HD), f32)
        for s in range(8):
            o = o + orecv[l, s].astype(f32) * cols[l * 64:(l + 1) * 64, s:s + 1]
        o = o.reshape(2, GROUP, 8, HD)
        both = [jnp.swapaxes(o[to], 0, 1) for to in range(2)]
        fsend[l] = jnp.stack(both, axis=1).reshape(16, GROUP, HD)
        for k in range(1, 16):
            to = (spot + k) % 16
            remote(fsend.at[l, to], frecv.at[l, spot], d_s.at[l], d_r.at[l],
                   at(to // 2, to % 2, z, c)).start()
        frecv[l, spot] = fsend[l, spot]

    cols = sources()
    combine(0, cols)
    combine(1, cols)

    def shares():
        remote(grecv.at[0:15], grecv.at[0:15], g_sem.at[0], g_sem.at[1]).wait_recv()
        g = grecv[...].reshape(KVH, 2, 8, HD)
        la, lb, lc = g[:, 0], g[:, 1], sbuf_l[...]
        top = jnp.maximum(jnp.maximum(la, lb), lc)
        a, b, s = jnp.exp2(la - top), jnp.exp2(lb - top), jnp.exp2(lc - top)
        den = a + b + s
        return a / den, b / den, s / den * sbuf_o[...]

    def finish(l, a, b, s):
        remote(frecv.at[l, 0:15], frecv.at[l, 0:15], d_s.at[l], d_r.at[l]).wait_recv()
        part_of = slice(l * GROUP, (l + 1) * GROUP)
        got = frecv[l].reshape(KVH, 2, GROUP, HD)
        return got[:, 0] * a[:, part_of] + got[:, 1] * b[:, part_of] + s[:, part_of]

    a, b, s = shares()
    o0 = finish(0, a, b, s)
    o1 = finish(1, a, b, s)
    for h in range(KVH):
        for g in range(GROUP):
            pair = jnp.concatenate([o0[h, g:g + 1], o1[h, g:g + 1]], axis=0)
            out[:, (h * GROUP + g) * HD:(h * GROUP + g + 1) * HD] = pair.astype(bf16)

    remote(qa.at[0:7], qa.at[0:7], a_sem.at[0], a_sem.at[1]).wait_send()
    remote(qall.at[0:7, 0], qall.at[0:7, 0], b_sem.at[0], b_sem.at[1]).wait_send()
    y_copy(yl).wait_send()
    remote(lrecv.at[0:7], lrecv.at[0:7], l_sem.at[0], l_sem.at[1]).wait_send()
    remote(grecv.at[0:15], grecv.at[0:15], g_sem.at[0], g_sem.at[1]).wait_send()
    for l in range(2):
        for k in range(2):
            remote(kown.at[l, k, 0:7], kown.at[l, k, 0:7], kv_s.at[l * 2 + k], kv_r.at[0]).wait_send()
            forward(l, k).wait_send()
        remote(orecv.at[l, 0:7], orecv.at[l, 0:7], c_s.at[l], c_r.at[l]).wait_send()
        remote(frecv.at[l, 0:15], frecv.at[l, 0:15], d_s.at[l], d_r.at[l]).wait_send()


def body(prefix_cache, queries, suffix_cache, suffix_lengths, slot_request):
    bf, f32 = jnp.bfloat16, jnp.float32
    dma = pltpu.SemaphoreType.DMA
    any_space = pl.BlockSpec(memory_space=pl.ANY)
    out = pl.pallas_call(
        kernel,
        out_shape=jax.ShapeDtypeStruct((2, QH * HD), bf),
        in_specs=[
            any_space,
            any_space,
            any_space,
            pl.BlockSpec(memory_space=pltpu.SMEM),
            pl.BlockSpec(memory_space=pltpu.SMEM),
        ],
        out_specs=pl.BlockSpec(memory_space=pltpu.VMEM),
        scratch_shapes=[
            pltpu.VMEM((2, 2, 16, 8192), bf),
            pltpu.VMEM((2, 2, 8, 16, POS), bf),
            pltpu.VMEM((2, 2, 8, 16, POS), bf),
            pltpu.VMEM((2, 1, 2, SUF, KVH * HD), bf),
            pltpu.VMEM((2, QH * HD), bf),
            pltpu.VMEM((8, 8, HD), bf),
            pltpu.VMEM((8, 8, HD), bf),
            pltpu.VMEM((8, 2, 64, HD), bf),
            pltpu.VMEM((2, 2, 512, POS), bf),
            pltpu.VMEM((2, 512, HD), f32),
            pltpu.VMEM((512, HD), f32),
            pltpu.VMEM((KVH, 8, HD), f32),
            pltpu.VMEM((KVH, 8, HD), f32),
            pltpu.VMEM((2, 8, 64, HD), bf),
            pltpu.VMEM((2, 8, 64, HD), bf),
            pltpu.VMEM((8, 1, HD), f32),
            pltpu.VMEM((8, 1, HD), f32),
            pltpu.VMEM((16, 8, HD), f32),
            pltpu.VMEM((16, 8, HD), f32),
            pltpu.VMEM((2, 16, GROUP, HD), f32),
            pltpu.VMEM((2, 16, GROUP, HD), f32),
            dma((10,)),
            dma((2,)), dma((2,)), dma((2,)),
            dma((4,)), dma((4,)), dma((8,)),
            dma((4,)), dma((4,)),
            dma((2,)), dma((2,)),
            dma((2,)), dma((2,)),
            dma((2,)), dma((2,)),
        ],
        compiler_params=pltpu.CompilerParams(collective_id=0, has_side_effects=True),
        name="attend",
    )(prefix_cache, queries.reshape(2, QH * HD), suffix_cache, suffix_lengths, slot_request)
    return out.reshape(2, 1, QH * HD)


def solution(mesh):
    in_specs = (
        P(None, None, "seq", "rep"),
        P(None, ("seq", "rep"), None),
        P(None, ("seq", "rep"), None, None, None),
        P(),
        P(("seq", "rep")),
    )
    out_specs = P(None, ("seq", "rep"), None)
    return jax.shard_map(body, mesh=mesh, in_specs=in_specs, out_specs=out_specs, check_vma=False)
```

```python
import math

import jax
import jax.numpy as jnp
from jax import lax
from jax.experimental import pallas as pl
from jax.experimental.pallas import tpu as pltpu
from jax.sharding import PartitionSpec as P

QH = 32
KVH = 8
HD = 128
SUF = 128
GROUP = 4
NEG = -1e30
SCALE2 = HD ** -0.5 * math.log2(math.e)
POS = 1024
HALF = POS // 2
NT = (((1,), (1,)), ((), ()))
NN = (((1,), (0,)), ((), ()))
MESH = pl.DeviceIdType.MESH


def dot(a, b, dims):
    return lax.dot_general(a, b, dims, preferred_element_type=jnp.float32)


def kernel(
    prefix, queries, suffix, lengths_in, slot_in, out,
    lengths, slot, stage, kown, koth, suf, qraw, qmsg, qa, qall, wbuf, rden, oacc, sbuf_o, sbuf_l,
    osend, orecv, lsend, lrecv, gsend, grecv, share,
    loc_sem, a_sem, b_sem, y_sem, kv_s, kv_r, v1_r, f_s, f_r, c_s, c_r, l_sem, g_sem,
):
    f32, bf16 = jnp.float32, jnp.bfloat16
    seq = lax.axis_index("seq")
    rep = lax.axis_index("rep")
    x, y, zl = seq // 16, (seq // 4) % 4, seq % 4
    yh, yl = y // 2, y % 2
    zh, c = rep // 2, rep % 2
    z = zh * 4 + zl
    head = x * 2 + yh
    part = yl * 4 + zl
    spot = head * 2 + yl

    def at(head_to, yl_to, z_to, c_to):
        x_to, yh_to = head_to // 2, head_to % 2
        return ((x_to * 4 + yh_to * 2 + yl_to) * 4 + z_to % 4, (z_to // 4) * 2 + c_to)

    other = at(head, yl, z, 1 - c)

    def remote(src, dst, s, r, dev=other):
        return pltpu.make_async_remote_copy(
            src_ref=src, dst_ref=dst, send_sem=s, recv_sem=r, device_id=dev, device_id_type=MESH)

    load_q = pltpu.make_async_copy(queries, qraw, loc_sem.at[9])
    load_q.start()
    barrier = pltpu.get_barrier_semaphore()
    peers = [other]
    for k in range(1, 16):
        to = (spot + k) % 16
        peers.append(at(to // 2, to % 2, z, c))
    for k in range(1, 8):
        peers.append(at(head, yl, (z + k) % 8, c))
    for k in range(1, 4):
        peers.append(at(head, 1 - yl, zh * 4 + (zl + k) % 4, c))
    for dev in peers:
        pl.semaphore_signal(barrier, inc=1, device_id=dev, device_id_type=MESH)

    order = ((0, 0), (1, 0), (0, 1), (1, 1))
    loads = {(l, k): pltpu.make_async_copy(prefix.at[l, k], stage.at[l, k], loc_sem.at[l * 2 + k])
             for l, k in order}
    owns = {(l, k): pltpu.make_async_copy(
        prefix.at[l, k, :, pl.ds(pl.multiple_of(part * POS, POS), POS)],
        kown.at[l, k, part], loc_sem.at[4 + l * 2 + k]) for l, k in order}
    load_suf = pltpu.make_async_copy(suffix, suf, loc_sem.at[8])
    load_len = pltpu.make_async_copy(lengths_in, lengths, loc_sem.at[10])
    load_slot = pltpu.make_async_copy(slot_in, slot, loc_sem.at[11])
    loads[0, 0].start()
    load_suf.start()
    load_len.start()
    load_slot.start()

    for l, k in order:
        if (l, k) != (0, 0):
            loads[l, k].start()
        owns[l, k].start()

    load_q.wait()
    q32 = qraw[...].astype(f32)
    for h in range(KVH):
        rows = [q32[l:l + 1, (h * GROUP + g) * HD:(h * GROUP + g + 1) * HD]
                for l in range(2) for g in range(GROUP)]
        qmsg[h] = jnp.concatenate(rows, axis=0).astype(bf16)
    loads[0, 0].wait()
    pl.semaphore_wait(barrier, len(peers))

    for k in range(1, 8):
        to = (head + k) % 8
        remote(qmsg.at[to], qa.at[head], a_sem.at[0], a_sem.at[1], at(to, yl, z, c)).start()
    qa[head] = qmsg[head]

    def kv_send(l, k, steps, half=None):
        for dz, dy in steps:
            yl_to, zl_to = (yl + dy) % 2, (zl + dz) % 4
            to = yl_to * 4 + zl_to
            if half is None:
                start, size, dst, r = 0, POS, kown.at[l, k, part], kv_r.at[l * 2 + k]
            else:
                start, size = half * HALF, HALF
                dst = kown.at[l, k, part, :, start:start + HALF]
                r = v1_r.at[part] if half else kv_r.at[l * 2 + k]
            remote(
                stage.at[l, k, :, pl.ds(pl.multiple_of(to * POS + start, HALF), size)],
                dst, kv_s.at[l * 2 + k], r, at(head, yl_to, zh * 4 + zl_to, c)).start()

    def kv_wait(l, k):
        owns[l, k].wait()
        remote(kown.at[l, k, 0:7], kown.at[l, k, 0:7], kv_s.at[0], kv_r.at[l * 2 + k]).wait_recv()

    def forward(l, k):
        return remote(kown.at[l, k], koth.at[l, k], f_s.at[l * 2 + k], f_r.at[l * 2 + k])

    full = [(2, 0), (2, 1), (1, 0), (1, 1), (3, 0), (3, 1), (0, 1)]

    kv_send(0, 0, [(2, 0), (2, 1), (0, 1), (1, 0)])

    load_suf.wait()
    load_len.wait()
    load_slot.wait()
    count = lengths[slot[0]]
    row = lax.broadcasted_iota(jnp.int32, (8, HD), 0)
    lane = lax.broadcasted_iota(jnp.int32, (8, HD), 1)
    valid = lane < count

    def suffix_head(h):
        cols = slice(h * HD, (h + 1) * HD)
        q = qmsg[h]
        s0 = dot(q, suf[0, 0, 0, :, cols], NT)
        s1 = dot(q, suf[1, 0, 0, :, cols], NT)
        s = jnp.where(valid, jnp.where(row < GROUP, s0, s1) * SCALE2, NEG)
        top = jnp.max(s, axis=1, keepdims=True)
        w = jnp.where(valid, jnp.exp2(s - top), 0.0).astype(bf16)
        den = jnp.sum(w.astype(f32), axis=1, keepdims=True)
        n0 = dot(w, suf[0, 0, 1, :, cols], NN)
        n1 = dot(w, suf[1, 0, 1, :, cols], NN)
        sbuf_o[h] = jnp.where(row < GROUP, n0, n1) / den
        sbuf_l[h] = jnp.broadcast_to(top + jnp.log2(den), (8, HD))

    def suffix_part():
        for h in range(KVH):
            suffix_head(h)

    suffix_part()

    def a_wait():
        remote(qa.at[0:7], qa.at[0:7], a_sem.at[0], a_sem.at[1]).wait_recv()

    a_wait()
    low = row < GROUP

    def regroup(a, b):
        return (jnp.where(low, a, pltpu.roll(b, GROUP, 0)), jnp.where(low, pltpu.roll(a, GROUP, 0), b))

    pairs = [regroup(qa[2 * j].astype(f32), qa[2 * j + 1].astype(f32)) for j in range(4)]
    qall[z, yl] = jnp.concatenate([p[l] for l in range(2) for p in pairs], axis=0).astype(bf16)
    line = (z + 2) % 8

    def mate(k):
        return (line // 4 * 4 + (line + k) % 4 + 6) % 8

    mirror = zh * 4 + 3 - zl

    def b_send(block, z_to, r):
        remote(qall.at[block, yl], qall.at[block, yl], b_sem.at[0], r, at(head, yl, z_to, c)).start()

    b_send(z, mirror, b_sem.at[2])
    for k in (2, 1, 3):
        b_send(z, mate(k), b_sem.at[1])
    loads[1, 0].wait()
    kv_send(0, 0, [(1, 1), (3, 0), (3, 1)])
    kv_send(1, 0, [(2, 0)])

    def m_wait():
        remote(qall.at[mirror, yl], qall.at[mirror, yl], b_sem.at[0], b_sem.at[2]).wait_recv()

    m_wait()
    for k in (2, 1, 3):
        b_send(mirror, mate(k), b_sem.at[1])
    loads[0, 1].wait()
    kv_send(1, 0, full[1:])
    kv_send(0, 1, full[:2])
    kv_wait(0, 0)
    forward(0, 0).start()

    def b_wait():
        remote(qall.at[0:6, 0], qall.at[0:6, 0], b_sem.at[0], b_sem.at[1]).wait_recv()

    def y_copy(which):
        return remote(qall.at[:, which], qall.at[:, which], y_sem.at[0], y_sem.at[1],
                      at(head, 1 - yl, z, c))

    def y_wait():
        y_copy(1 - yl).wait_recv()

    b_wait()
    y_copy(yl).start()
    kv_send(0, 1, full[2:])
    loads[1, 1].wait()

    def weights(l):
        forward(l, 0).wait_recv()
        r64 = lax.broadcasted_iota(jnp.int32, (2, 64, HD), 1)
        c64 = lax.broadcasted_iota(jnp.int32, (2, 64, HD), 2)

        def rows(i, carry):
            q = qall[pl.ds(i * 2, 2), :, l * 32:(l + 1) * 32, :].reshape(128, HD)
            at_rows = pl.ds(pl.multiple_of(i * 128, 128), 128)
            sa = dot(q, kown[l, 0].reshape(HD, POS), NN) * SCALE2
            sb = dot(q, koth[l, 0].reshape(HD, POS), NN) * SCALE2
            top = jnp.maximum(jnp.max(sa, axis=1, keepdims=True), jnp.max(sb, axis=1, keepdims=True))
            wa = jnp.exp2(sa - top).astype(bf16)
            wb = jnp.exp2(sb - top).astype(bf16)
            den = jnp.sum(wa.astype(f32) + wb.astype(f32), axis=1, keepdims=True)
            wbuf[l, 0, at_rows, :] = wa
            wbuf[l, 1, at_rows, :] = wb
            rden[l, at_rows, :] = jnp.broadcast_to(1.0 / den, (128, HD))
            big = jnp.broadcast_to(top + jnp.log2(den), (128, HD)).reshape(2, 64, HD)
            line = jnp.sum(jnp.where(c64 == r64 + l * 64, big, 0.0), axis=1, keepdims=True)
            if l == 0:
                lsend[pl.ds(i * 2, 2)] = line
            else:
                lsend[pl.ds(i * 2, 2)] = lsend[pl.ds(i * 2, 2)] + line
            return carry

        lax.fori_loop(0, 4, rows, 0, unroll=True)

    def partials(l):
        def ring(j, carry):
            dz = 4 + (j + 1) // 2 * (1 - 2 * (j % 2))
            z_to = (z + dz) % 8
            for i in range(15, -1, -1):
                spot_to = (spot + i) % 16
                copy = remote(
                    osend.at[l, z_to * 16 + spot_to % 2 * 8 + spot_to // 2], orecv.at[l, spot * 8 + z],
                    c_s.at[l], c_r.at[l], at(spot_to // 2, spot_to % 2, z_to, c))
                if i:
                    copy.start()
                else:
                    pl.when(dz != 0)(copy.start)
            return carry

        lax.fori_loop(0, 8, ring, 0)
        orecv[l, spot * 8 + z] = osend[l, z * 16 + yl * 8 + head]

    def store_partials(l, o):
        osend.at[l].reshape(512, HD)[...] = o.astype(bf16)

    def values_own(l):
        oacc[l] = dot(wbuf[l, 0], kown[l, 1].reshape(HD, POS), NT)

    def values_other(l):
        forward(l, 1).wait_recv()
        store_partials(l, (oacc[l] + dot(wbuf[l, 1], koth[l, 1].reshape(HD, POS), NT)) * rden[l])

    def sources():
        remote(lrecv.at[0:7], lrecv.at[0:7], l_sem.at[0], l_sem.at[1]).wait_recv()
        ls = jnp.concatenate([lrecv[...].reshape(8, HD), jnp.full((120, HD), NEG, f32)], axis=0).T
        for half in range(2):
            for j in range(4):
                base = half * 32 + j * 8
                even, odd = regroup(ls[base:base + 8], ls[64 + base:72 + base])
                gsend[4 * j + half] = even
                gsend[4 * j + 2 + half] = odd
        for k in range(1, 16):
            to = (spot + k) % 16
            remote(gsend.at[to], grecv.at[spot], g_sem.at[0], g_sem.at[1],
                   at(to // 2, to % 2, z, c)).start()
        grecv[spot] = gsend[spot]

    kv_wait(1, 0)
    forward(1, 0).start()
    kv_send(1, 1, full, 0)
    y_wait()
    weights(0)
    kv_send(1, 1, full, 1)
    weights(1)
    for k in range(1, 8):
        to = (z + k) % 8
        remote(lsend.at[to], lrecv.at[z], l_sem.at[0], l_sem.at[1], at(head, yl, to, c)).start()
    lrecv[z] = lsend[z]
    kv_wait(0, 1)
    forward(0, 1).start()
    values_own(0)

    first, second = slice(0, HALF), slice(HALF, POS)

    def last_first():
        owns[1, 1].wait()
        piece = kown.at[1, 1, 0:7, :, first]
        remote(piece, piece, kv_s.at[0], kv_r.at[3]).wait_recv()

    def last_copy():
        return remote(kown.at[1, 1, :, :, first], koth.at[1, 1, :, :, first], f_s.at[4], f_r.at[4])

    def last_dot(which, ref, span):
        return dot(wbuf[1, which, :, span], ref[1, 1, :, :, span].reshape(HD, HALF), NT)

    def values_first():
        oacc[1] = last_dot(0, kown, first)

    def last_pieces():
        own = kown.at[1, 1, part, :, second]
        remote(own, koth.at[1, 1, part, :, second], f_s.at[3], f_r.at[3]).start()
        for dz, dy in full:
            src = (yl + dy) % 2 * 4 + (zl + 4 - dz) % 4
            piece = kown.at[1, 1, src, :, second]
            remote(piece, piece, kv_s.at[0], v1_r.at[src]).wait_recv()
            remote(piece, koth.at[1, 1, src, :, second], f_s.at[3], f_r.at[3]).start()

    def values_second():
        oacc[1] = oacc[1] + last_dot(0, kown, second)
        last_copy().wait_recv()
        oacc[1] = oacc[1] + last_dot(1, koth, first)
        whole = koth.at[1, 1, :, :, second]
        remote(whole, whole, f_s.at[3], f_r.at[3]).wait_recv()
        store_partials(1, (oacc[1] + last_dot(1, koth, second)) * rden[1])

    last_first()
    last_copy().start()
    values_first()
    values_other(0)
    partials(0)
    last_pieces()
    sources()
    values_second()
    partials(1)

    def shares():
        remote(grecv.at[0:15], grecv.at[0:15], g_sem.at[0], g_sem.at[1]).wait_recv()

        def one_head(h, carry):
            la, lb, lc = grecv[2 * h], grecv[2 * h + 1], sbuf_l[h]
            top = jnp.max(jnp.maximum(jnp.maximum(la, lb), lc), axis=1, keepdims=True)
            a, b, s = jnp.exp2(la - top), jnp.exp2(lb - top), jnp.exp2(lc - top)
            den = jnp.sum(a + b, axis=1, keepdims=True) + s
            sbuf_o[h] = s / den * sbuf_o[h]
            for half, w in enumerate((a / den, b / den)):
                for j in range(4):
                    pair = [jnp.broadcast_to(w[:, k:k + 1], (8, HD)) for k in (2 * j, 2 * j + 1)]
                    for l, tile in enumerate(regroup(*pair)):
                        share[l, 2 * h + half, j] = tile
            return carry

        lax.fori_loop(0, KVH, one_head, 0)

    def finish(l):
        remote(orecv.at[l, 0:127], orecv.at[l, 0:127], c_s.at[l], c_r.at[l]).wait_recv()
        got = orecv.at[l].reshape(512, HD)[...].astype(f32).reshape(KVH, 8, 8, HD)
        return jnp.sum(got * share[l].reshape(KVH, 8, 8, HD), axis=1)

    shares()
    o0 = finish(0)
    o1 = finish(1)
    for h in range(KVH):
        first_half, last_half = regroup(o0[h], o1[h])
        both = first_half + last_half + sbuf_o[h]
        for g in range(GROUP):
            pair = jnp.concatenate([both[g:g + 1], both[GROUP + g:GROUP + g + 1]], axis=0)
            out[:, (h * GROUP + g) * HD:(h * GROUP + g + 1) * HD] = pair.astype(bf16)

    remote(qa.at[0:7], qa.at[0:7], a_sem.at[0], a_sem.at[1]).wait_send()
    remote(qall.at[0:7, 0], qall.at[0:7, 0], b_sem.at[0], b_sem.at[1]).wait_send()
    y_copy(yl).wait_send()
    last_copy().wait_send()
    remote(kown.at[1, 1, :, :, second], koth.at[1, 1, :, :, second], f_s.at[3], f_r.at[3]).wait_send()
    remote(lrecv.at[0:7], lrecv.at[0:7], l_sem.at[0], l_sem.at[1]).wait_send()
    remote(grecv.at[0:15], grecv.at[0:15], g_sem.at[0], g_sem.at[1]).wait_send()
    for l in range(2):
        for k in range(2):
            remote(kown.at[l, k, 0:7], kown.at[l, k, 0:7], kv_s.at[l * 2 + k], kv_r.at[0]).wait_send()
            if (l, k) != (1, 1):
                forward(l, k).wait_send()
        remote(orecv.at[l, 0:127], orecv.at[l, 0:127], c_s.at[l], c_r.at[l]).wait_send()


def body(prefix_cache, queries, suffix_cache, suffix_lengths, slot_request):
    bf, f32 = jnp.bfloat16, jnp.float32
    dma = pltpu.SemaphoreType.DMA
    any_space = pl.BlockSpec(memory_space=pl.ANY)
    out = pl.pallas_call(
        kernel,
        out_shape=pltpu.VMEM((2, QH * HD), bf),
        in_specs=[
            any_space,
            any_space,
            any_space,
            any_space,
            any_space,
        ],
        out_specs=pl.BlockSpec(memory_space=pltpu.VMEM),
        scratch_shapes=[
            pltpu.SMEM((256,), jnp.int32),
            pltpu.SMEM((1,), jnp.int32),
            pltpu.VMEM((2, 2, 16, 8192), bf),
            pltpu.VMEM((2, 2, 8, 16, POS), bf),
            pltpu.VMEM((2, 2, 8, 16, POS), bf),
            pltpu.VMEM((2, 1, 2, SUF, KVH * HD), bf),
            pltpu.VMEM((2, QH * HD), bf),
            pltpu.VMEM((8, 8, HD), bf),
            pltpu.VMEM((8, 8, HD), bf),
            pltpu.VMEM((8, 2, 64, HD), bf),
            pltpu.VMEM((2, 2, 512, POS), bf),
            pltpu.VMEM((2, 512, HD), f32),
            pltpu.VMEM((2, 512, HD), f32),
            pltpu.VMEM((KVH, 8, HD), f32),
            pltpu.VMEM((KVH, 8, HD), f32),
            pltpu.VMEM((2, 128, GROUP, HD), bf),
            pltpu.VMEM((2, 128, GROUP, HD), bf),
            pltpu.VMEM((8, 1, HD), f32),
            pltpu.VMEM((8, 1, HD), f32),
            pltpu.VMEM((16, 8, HD), f32),
            pltpu.VMEM((16, 8, HD), f32),
            pltpu.VMEM((2, 16, 4, 8, HD), f32),
            dma((12,)),
            dma((2,)), dma((3,)), dma((2,)),
            dma((4,)), dma((4,)), dma((8,)),
            dma((5,)), dma((5,)),
            dma((2,)), dma((2,)),
            dma((2,)), dma((2,)),
        ],
        compiler_params=pltpu.CompilerParams(collective_id=0, has_side_effects=True),
        name="attend",
    )(prefix_cache, queries.reshape(2, QH * HD), suffix_cache, suffix_lengths, slot_request)
    return out.reshape(2, 1, QH * HD)


def solution(mesh):
    in_specs = (
        P(None, None, "seq", "rep"),
        P(None, ("seq", "rep"), None),
        P(None, ("seq", "rep"), None, None, None),
        P(),
        P(("seq", "rep")),
    )
    out_specs = P(None, ("seq", "rep"), None)
    return jax.shard_map(body, mesh=mesh, in_specs=in_specs, out_specs=out_specs, check_vma=False)
```

```python
import math

import jax
import jax.numpy as jnp
from jax import lax
from jax.experimental import pallas as pl
from jax.experimental.pallas import tpu as pltpu
from jax.sharding import PartitionSpec as P

QH = 32
KVH = 8
HD = 128
SUF = 128
GROUP = 4
NEG = -1e30
SCALE2 = HD ** -0.5 * math.log2(math.e)
POS = 1024
HALF = POS // 2
NT = (((1,), (1,)), ((), ()))
NN = (((1,), (0,)), ((), ()))
MESH = pl.DeviceIdType.MESH
OFFSETS = sorted(
    [(dz, dx, dy) for dz in range(8) for dx in range(4) for dy in range(4) if dz + dx + dy],
    key=lambda o: -(min(o[0], 8 - o[0]) + min(o[1], 4 - o[1]) + min(o[2], 4 - o[2])))
FAR, NEAR = OFFSETS[:64], OFFSETS[64:]


def dot(a, b, dims):
    return lax.dot_general(a, b, dims, preferred_element_type=jnp.float32)


def kernel(
    prefix, queries, suffix, lengths_in, slot_in, out,
    lengths, slot, stage, kown, koth, suf, qraw, qmsg, qa, qall, wbuf, rden, oacc, sbuf_o, sbuf_l,
    osend, orecv, lsend, lrecv, gsend, grecv, share,
    loc_sem, a_sem, b_sem, y_sem, kv_s, kv_r, v1_r, f_s, f_r, c_s, c_r, l_sem, g_sem,
):
    f32, bf16 = jnp.float32, jnp.bfloat16
    seq = lax.axis_index("seq")
    rep = lax.axis_index("rep")
    x, y, zl = seq // 16, (seq // 4) % 4, seq % 4
    yh, yl = y // 2, y % 2
    zh, c = rep // 2, rep % 2
    z = zh * 4 + zl
    head = x * 2 + yh
    part = yl * 4 + zl
    spot = head * 2 + yl

    def at(head_to, yl_to, z_to, c_to):
        x_to, yh_to = head_to // 2, head_to % 2
        return ((x_to * 4 + yh_to * 2 + yl_to) * 4 + z_to % 4, (z_to // 4) * 2 + c_to)

    other = at(head, yl, z, 1 - c)

    def remote(src, dst, s, r, dev=other):
        return pltpu.make_async_remote_copy(
            src_ref=src, dst_ref=dst, send_sem=s, recv_sem=r, device_id=dev, device_id_type=MESH)

    load_q = pltpu.make_async_copy(queries, qraw, loc_sem.at[9])
    load_first = pltpu.make_async_copy(prefix.at[0, 0], stage.at[0, 0], loc_sem.at[0])
    load_first.start()
    load_q.start()
    barrier = pltpu.get_barrier_semaphore()
    line = (z + 2) % 8

    def mate(k):
        return (line // 4 * 4 + (line + k) % 4 + 6) % 8

    peers = [other, at(head, 1 - yl, z, c)]
    for k in range(1, 8):
        peers.append(at((head + k) % 8, yl, z, c))
    for k in range(1, 4):
        peers.append(at(head, yl, zh * 4 + (zl + k) % 4, c))
        peers.append(at(head, 1 - yl, zh * 4 + (zl + k) % 4, c))
    for k in range(2):
        peers.append(at(head, yl, (line // 4 * 4 + (line % 4 // 2 * 2 + 2 + k) % 4 + 6) % 8, c))
    for dev in peers:
        pl.semaphore_signal(barrier, inc=1, device_id=dev, device_id_type=MESH)

    order = ((0, 0), (1, 0), (0, 1), (1, 1))
    loads = {(l, k): pltpu.make_async_copy(prefix.at[l, k], stage.at[l, k], loc_sem.at[l * 2 + k])
             for l, k in order}
    owns = {(l, k): pltpu.make_async_copy(
        prefix.at[l, k, :, pl.ds(pl.multiple_of(part * POS, POS), POS)],
        kown.at[l, k, part], loc_sem.at[4 + l * 2 + k]) for l, k in order}
    load_suf = pltpu.make_async_copy(suffix, suf, loc_sem.at[8])
    load_len = pltpu.make_async_copy(lengths_in, lengths, loc_sem.at[10])
    load_slot = pltpu.make_async_copy(slot_in, slot, loc_sem.at[11])
    load_suf.start()
    load_len.start()
    load_slot.start()

    for l, k in order:
        if (l, k) != (0, 0):
            loads[l, k].start()
        owns[l, k].start()

    load_q.wait()
    q32 = qraw[...].astype(f32)
    for h in range(KVH):
        rows = [q32[l:l + 1, (h * GROUP + g) * HD:(h * GROUP + g + 1) * HD]
                for l in range(2) for g in range(GROUP)]
        qmsg[h] = jnp.concatenate(rows, axis=0).astype(bf16)
    pl.semaphore_wait(barrier, len(peers))

    for k in range(1, 8):
        to = (head + k) % 8
        remote(qmsg.at[to], qa.at[head], a_sem.at[0], a_sem.at[1], at(to, yl, z, c)).start()
    qa[head] = qmsg[head]

    def kv_send(l, k, steps, half=None):
        for dz, dy in steps:
            yl_to, zl_to = (yl + dy) % 2, (zl + dz) % 4
            to = yl_to * 4 + zl_to
            if half is None:
                start, size, dst, r = 0, POS, kown.at[l, k, part], kv_r.at[l * 2 + k]
            else:
                start, size = half * HALF, HALF
                dst = kown.at[l, k, part, :, start:start + HALF]
                r = v1_r.at[part] if half else kv_r.at[l * 2 + k]
            remote(
                stage.at[l, k, :, pl.ds(pl.multiple_of(to * POS + start, HALF), size)],
                dst, kv_s.at[l * 2 + k], r, at(head, yl_to, zh * 4 + zl_to, c)).start()

    def kv_wait(l, k):
        owns[l, k].wait()
        remote(kown.at[l, k, 0:7], kown.at[l, k, 0:7], kv_s.at[0], kv_r.at[l * 2 + k]).wait_recv()

    def forward(l, k):
        return remote(kown.at[l, k], koth.at[l, k], f_s.at[l * 2 + k], f_r.at[l * 2 + k])

    full = [(2, 0), (2, 1), (1, 0), (1, 1), (3, 0), (3, 1), (0, 1)]

    load_first.wait()
    kv_send(0, 0, [(2, 0), (2, 1), (0, 1), (1, 0)])

    load_suf.wait()
    load_len.wait()
    load_slot.wait()
    count = lengths[slot[0]]
    row = lax.broadcasted_iota(jnp.int32, (8, HD), 0)
    lane = lax.broadcasted_iota(jnp.int32, (8, HD), 1)
    valid = lane < count

    def suffix_head(h):
        cols = slice(h * HD, (h + 1) * HD)
        q = qmsg[h]
        s0 = dot(q, suf[0, 0, 0, :, cols], NT)
        s1 = dot(q, suf[1, 0, 0, :, cols], NT)
        s = jnp.where(valid, jnp.where(row < GROUP, s0, s1) * SCALE2, NEG)
        top = jnp.max(s, axis=1, keepdims=True)
        w = jnp.where(valid, jnp.exp2(s - top), 0.0).astype(bf16)
        den = jnp.sum(w.astype(f32), axis=1, keepdims=True)
        n0 = dot(w, suf[0, 0, 1, :, cols], NN)
        n1 = dot(w, suf[1, 0, 1, :, cols], NN)
        sbuf_o[h] = jnp.where(row < GROUP, n0, n1) / den
        sbuf_l[h] = jnp.broadcast_to(top + jnp.log2(den), (8, HD))

    def suffix_part():
        for h in range(KVH):
            suffix_head(h)

    suffix_part()

    def a_wait():
        remote(qa.at[0:7], qa.at[0:7], a_sem.at[0], a_sem.at[1]).wait_recv()

    a_wait()
    low = row < GROUP

    def regroup(a, b):
        return (jnp.where(low, a, pltpu.roll(b, GROUP, 0)), jnp.where(low, pltpu.roll(a, GROUP, 0), b))

    pairs = [regroup(qa[2 * j].astype(f32), qa[2 * j + 1].astype(f32)) for j in range(4)]
    qall[z, yl] = jnp.concatenate([p[l] for l in range(2) for p in pairs], axis=0).astype(bf16)
    mirror = zh * 4 + 3 - zl

    def b_send(block, z_to, r):
        remote(qall.at[block, yl], qall.at[block, yl], b_sem.at[0], r, at(head, yl, z_to, c)).start()

    def y_send(z_of):
        block = qall.at[z_of, yl]
        remote(block, block, y_sem.at[0], y_sem.at[1], at(head, 1 - yl, z, c)).start()

    b_send(z, mirror, b_sem.at[2])
    for k in (2, 1, 3):
        b_send(z, mate(k), b_sem.at[1])
    y_send(z)
    loads[1, 0].wait()
    kv_send(0, 0, [(1, 1), (3, 0), (3, 1)])
    kv_send(1, 0, [(2, 0)])

    def m_wait():
        remote(qall.at[mirror, yl], qall.at[mirror, yl], b_sem.at[0], b_sem.at[2]).wait_recv()

    m_wait()
    for k in (2, 1, 3):
        b_send(mirror, mate(k), b_sem.at[3])
    y_send(mirror)
    loads[0, 1].wait()
    kv_send(1, 0, full[1:])
    kv_send(0, 1, full[:2])
    kv_wait(0, 0)
    forward(0, 0).start()

    def b_wait(r):
        remote(qall.at[0:3, 0], qall.at[0:3, 0], b_sem.at[0], b_sem.at[r]).wait_recv()

    def y_wait():
        whole = qall.at[:, 1 - yl]
        remote(whole, whole, y_sem.at[0], y_sem.at[1]).wait_recv()

    b_wait(1)
    for k in range(1, 4):
        y_send(mate(k))
    kv_send(0, 1, full[2:5])
    b_wait(3)
    for k in range(1, 4):
        y_send(mate(k) // 4 * 4 + 3 - mate(k) % 4)
    kv_send(0, 1, full[5:])
    loads[1, 1].wait()

    def weights(l):
        forward(l, 0).wait_recv()
        r64 = lax.broadcasted_iota(jnp.int32, (2, 64, HD), 1)
        c64 = lax.broadcasted_iota(jnp.int32, (2, 64, HD), 2)

        def rows(i, carry):
            q = qall[pl.ds(i * 2, 2), :, l * 32:(l + 1) * 32, :].reshape(128, HD)
            at_rows = pl.ds(pl.multiple_of(i * 128, 128), 128)
            sa = dot(q, kown[l, 0].reshape(HD, POS), NN) * SCALE2
            sb = dot(q, koth[l, 0].reshape(HD, POS), NN) * SCALE2
            top = jnp.maximum(jnp.max(sa, axis=1, keepdims=True), jnp.max(sb, axis=1, keepdims=True))
            wa = jnp.exp2(sa - top).astype(bf16)
            wb = jnp.exp2(sb - top).astype(bf16)
            den = jnp.sum(wa.astype(f32) + wb.astype(f32), axis=1, keepdims=True)
            wbuf[l, 0, at_rows, :] = wa
            wbuf[l, 1, at_rows, :] = wb
            rden[l, at_rows, :] = jnp.broadcast_to(1.0 / den, (128, HD))
            big = jnp.broadcast_to(top + jnp.log2(den), (128, HD)).reshape(2, 64, HD)
            line = jnp.sum(jnp.where(c64 == r64 + l * 64, big, 0.0), axis=1, keepdims=True)
            if l == 0:
                lsend[pl.ds(i * 2, 2)] = line
            else:
                lsend[pl.ds(i * 2, 2)] = lsend[pl.ds(i * 2, 2)] + line
            return carry

        lax.fori_loop(0, 4, rows, 0, unroll=True)

    z_at = [(z + d) % 8 for d in range(8)]
    x_at = [(x + d) % 4 for d in range(4)]
    y_at = [(y + d) % 4 for d in range(4)]

    def partials(l, offsets):
        for dz, dx, dy in offsets:
            z_to, x_to, y_to = z_at[dz], x_at[dx], y_at[dy]
            dev = ((x_to * 4 + y_to) * 4 + z_to % 4, z_to // 4 * 2 + c)
            remote(osend.at[l, z_to * 16 + y_to % 2 * 8 + x_to * 2 + y_to // 2],
                   orecv.at[l, spot * 8 + z], c_s.at[l], c_r.at[l], dev).start()

    def store_partials(l, o):
        osend.at[l].reshape(512, HD)[...] = o.astype(bf16)
        orecv[l, spot * 8 + z] = osend[l, z * 16 + yl * 8 + head]

    def values_own(l):
        oacc[l] = dot(wbuf[l, 0], kown[l, 1].reshape(HD, POS), NT)

    def values_other(l):
        forward(l, 1).wait_recv()
        store_partials(l, (oacc[l] + dot(wbuf[l, 1], koth[l, 1].reshape(HD, POS), NT)) * rden[l])

    def sources():
        remote(lrecv.at[0:7], lrecv.at[0:7], l_sem.at[0], l_sem.at[1]).wait_recv()
        ls = jnp.concatenate([lrecv[...].reshape(8, HD), jnp.full((120, HD), NEG, f32)], axis=0).T
        for half in range(2):
            for j in range(4):
                base = half * 32 + j * 8
                even, odd = regroup(ls[base:base + 8], ls[64 + base:72 + base])
                gsend[4 * j + half] = even
                gsend[4 * j + 2 + half] = odd
        for k in range(1, 16):
            to = (spot + k) % 16
            remote(gsend.at[to], grecv.at[spot], g_sem.at[0], g_sem.at[1],
                   at(to // 2, to % 2, z, c)).start()
        grecv[spot] = gsend[spot]

    kv_wait(1, 0)
    forward(1, 0).start()
    kv_send(1, 1, full, 0)
    y_wait()
    weights(0)
    kv_send(1, 1, full, 1)
    weights(1)
    for k in range(1, 8):
        to = (z + k) % 8
        remote(lsend.at[to], lrecv.at[z], l_sem.at[0], l_sem.at[1], at(head, yl, to, c)).start()
    lrecv[z] = lsend[z]
    kv_wait(0, 1)
    forward(0, 1).start()
    values_own(0)

    first, second = slice(0, HALF), slice(HALF, POS)

    def last_first():
        owns[1, 1].wait()
        piece = kown.at[1, 1, 0:7, :, first]
        remote(piece, piece, kv_s.at[0], kv_r.at[3]).wait_recv()

    def last_copy():
        return remote(kown.at[1, 1, :, :, first], koth.at[1, 1, :, :, first], f_s.at[4], f_r.at[4])

    def last_dot(which, ref, span):
        return dot(wbuf[1, which, :, span], ref[1, 1, :, :, span].reshape(HD, HALF), NT)

    def values_first():
        oacc[1] = last_dot(0, kown, first)

    def last_pieces():
        own = kown.at[1, 1, part, :, second]
        remote(own, koth.at[1, 1, part, :, second], f_s.at[3], f_r.at[3]).start()
        for dz, dy in full:
            src = (yl + dy) % 2 * 4 + (zl + 4 - dz) % 4
            piece = kown.at[1, 1, src, :, second]
            remote(piece, piece, kv_s.at[0], v1_r.at[src]).wait_recv()
            remote(piece, koth.at[1, 1, src, :, second], f_s.at[3], f_r.at[3]).start()

    def values_second():
        oacc[1] = oacc[1] + last_dot(0, kown, second)
        last_copy().wait_recv()
        oacc[1] = oacc[1] + last_dot(1, koth, first)
        whole = koth.at[1, 1, :, :, second]
        remote(whole, whole, f_s.at[3], f_r.at[3]).wait_recv()
        store_partials(1, (oacc[1] + last_dot(1, koth, second)) * rden[1])

    values_other(0)
    last_first()
    last_copy().start()
    values_first()
    last_pieces()
    partials(0, FAR)
    values_second()
    partials(1, FAR)
    sources()
    partials(1, NEAR)
    partials(0, NEAR)

    def shares():
        remote(grecv.at[0:15], grecv.at[0:15], g_sem.at[0], g_sem.at[1]).wait_recv()

        def one_head(h, carry):
            la, lb, lc = grecv[2 * h], grecv[2 * h + 1], sbuf_l[h]
            top = jnp.max(jnp.maximum(jnp.maximum(la, lb), lc), axis=1, keepdims=True)
            a, b, s = jnp.exp2(la - top), jnp.exp2(lb - top), jnp.exp2(lc - top)
            den = jnp.sum(a + b, axis=1, keepdims=True) + s
            sbuf_o[h] = s / den * sbuf_o[h]
            for half, w in enumerate((a / den, b / den)):
                for j in range(4):
                    pair = [jnp.broadcast_to(w[:, k:k + 1], (8, HD)) for k in (2 * j, 2 * j + 1)]
                    for l, tile in enumerate(regroup(*pair)):
                        share[l, 2 * h + half, j] = tile
            return carry

        lax.fori_loop(0, KVH, one_head, 0)

    def finish(l):
        remote(orecv.at[l, 0:127], orecv.at[l, 0:127], c_s.at[l], c_r.at[l]).wait_recv()
        got = orecv.at[l].reshape(512, HD)[...].astype(f32).reshape(KVH, 8, 8, HD)
        return jnp.sum(got * share[l].reshape(KVH, 8, 8, HD), axis=1)

    shares()
    o0 = finish(0)
    o1 = finish(1)
    for h in range(KVH):
        first_half, last_half = regroup(o0[h], o1[h])
        both = first_half + last_half + sbuf_o[h]
        for g in range(GROUP):
            pair = jnp.concatenate([both[g:g + 1], both[GROUP + g:GROUP + g + 1]], axis=0)
            out[:, (h * GROUP + g) * HD:(h * GROUP + g + 1) * HD] = pair.astype(bf16)

    remote(qa.at[0:7], qa.at[0:7], a_sem.at[0], a_sem.at[1]).wait_send()
    remote(qall.at[0:7, 0], qall.at[0:7, 0], b_sem.at[0], b_sem.at[1]).wait_send()
    remote(qall.at[:, yl], qall.at[:, yl], y_sem.at[0], y_sem.at[1]).wait_send()
    last_copy().wait_send()
    remote(kown.at[1, 1, :, :, second], koth.at[1, 1, :, :, second], f_s.at[3], f_r.at[3]).wait_send()
    remote(lrecv.at[0:7], lrecv.at[0:7], l_sem.at[0], l_sem.at[1]).wait_send()
    remote(grecv.at[0:15], grecv.at[0:15], g_sem.at[0], g_sem.at[1]).wait_send()
    for l in range(2):
        for k in range(2):
            remote(kown.at[l, k, 0:7], kown.at[l, k, 0:7], kv_s.at[l * 2 + k], kv_r.at[0]).wait_send()
            if (l, k) != (1, 1):
                forward(l, k).wait_send()
        remote(orecv.at[l, 0:127], orecv.at[l, 0:127], c_s.at[l], c_r.at[l]).wait_send()


def body(prefix_cache, queries, suffix_cache, suffix_lengths, slot_request):
    bf, f32 = jnp.bfloat16, jnp.float32
    dma = pltpu.SemaphoreType.DMA
    any_space = pl.BlockSpec(memory_space=pl.ANY)
    out = pl.pallas_call(
        kernel,
        out_shape=pltpu.VMEM((2, QH * HD), bf),
        in_specs=[
            any_space,
            any_space,
            any_space,
            any_space,
            any_space,
        ],
        out_specs=pl.BlockSpec(memory_space=pltpu.VMEM),
        scratch_shapes=[
            pltpu.SMEM((256,), jnp.int32),
            pltpu.SMEM((1,), jnp.int32),
            pltpu.VMEM((2, 2, 16, 8192), bf),
            pltpu.VMEM((2, 2, 8, 16, POS), bf),
            pltpu.VMEM((2, 2, 8, 16, POS), bf),
            pltpu.VMEM((2, 1, 2, SUF, KVH * HD), bf),
            pltpu.VMEM((2, QH * HD), bf),
            pltpu.VMEM((8, 8, HD), bf),
            pltpu.VMEM((8, 8, HD), bf),
            pltpu.VMEM((8, 2, 64, HD), bf),
            pltpu.VMEM((2, 2, 512, POS), bf),
            pltpu.VMEM((2, 512, HD), f32),
            pltpu.VMEM((2, 512, HD), f32),
            pltpu.VMEM((KVH, 8, HD), f32),
            pltpu.VMEM((KVH, 8, HD), f32),
            pltpu.VMEM((2, 128, GROUP, HD), bf),
            pltpu.VMEM((2, 128, GROUP, HD), bf),
            pltpu.VMEM((8, 1, HD), f32),
            pltpu.VMEM((8, 1, HD), f32),
            pltpu.VMEM((16, 8, HD), f32),
            pltpu.VMEM((16, 8, HD), f32),
            pltpu.VMEM((2, 16, 4, 8, HD), f32),
            dma((12,)),
            dma((2,)), dma((4,)), dma((2,)),
            dma((4,)), dma((4,)), dma((8,)),
            dma((5,)), dma((5,)),
            dma((2,)), dma((2,)),
            dma((2,)), dma((2,)),
        ],
        compiler_params=pltpu.CompilerParams(collective_id=0, has_side_effects=True),
        name="attend",
    )(prefix_cache, queries.reshape(2, QH * HD), suffix_cache, suffix_lengths, slot_request)
    return out.reshape(2, 1, QH * HD)


def solution(mesh):
    in_specs = (
        P(None, None, "seq", "rep"),
        P(None, ("seq", "rep"), None),
        P(None, ("seq", "rep"), None, None, None),
        P(),
        P(("seq", "rep")),
    )
    out_specs = P(None, ("seq", "rep"), None)
    return jax.shard_map(body, mesh=mesh, in_specs=in_specs, out_specs=out_specs, check_vma=False)
```

```python
import math

import jax
import jax.numpy as jnp
from jax import lax
from jax.experimental import pallas as pl
from jax.experimental.pallas import tpu as pltpu
from jax.sharding import PartitionSpec as P

QH = 32
KVH = 8
HD = 128
SUF = 128
GROUP = 4
NEG = -1e30
SCALE2 = HD ** -0.5 * math.log2(math.e)
POS = 1024
HALF = POS // 2
NT = (((1,), (1,)), ((), ()))
NN = (((1,), (0,)), ((), ()))
MESH = pl.DeviceIdType.MESH
OFFSETS = sorted(
    [(dz, dx, dy) for dz in range(8) for dx in range(4) for dy in range(4) if dz + dx + dy],
    key=lambda o: -(min(o[0], 8 - o[0]) + min(o[1], 4 - o[1]) + min(o[2], 4 - o[2])))
FAR, NEAR = OFFSETS[:64], OFFSETS[64:]


def dot(a, b, dims):
    return lax.dot_general(a, b, dims, preferred_element_type=jnp.float32)


def kernel(
    prefix, queries, suffix, lengths_in, slot_in, out,
    lengths, slot, stage, kown, koth, suf, qraw, qmsg, qa, qall, wbuf, rden, oacc, sbuf_o, sbuf_l,
    osend, orecv, lsend, hsend, lrecv, gsend, grecv, lfin, share,
    loc_sem, a_sem, b_sem, y_sem, kv_s, kv_r, v1_r, f_s, f_r, c_s, c_r, l_sem, g_sem,
):
    f32, bf16 = jnp.float32, jnp.bfloat16
    seq = lax.axis_index("seq")
    rep = lax.axis_index("rep")
    x, y, zl = seq // 16, (seq // 4) % 4, seq % 4
    yh, yl = y // 2, y % 2
    zh, c = rep // 2, rep % 2
    z = zh * 4 + zl
    head = x * 2 + yh
    part = yl * 4 + zl
    spot = head * 2 + yl

    def at(head_to, yl_to, z_to, c_to):
        x_to, yh_to = head_to // 2, head_to % 2
        return ((x_to * 4 + yh_to * 2 + yl_to) * 4 + z_to % 4, (z_to // 4) * 2 + c_to)

    other = at(head, yl, z, 1 - c)

    def remote(src, dst, s, r, dev=other):
        return pltpu.make_async_remote_copy(
            src_ref=src, dst_ref=dst, send_sem=s, recv_sem=r, device_id=dev, device_id_type=MESH)

    load_q = pltpu.make_async_copy(queries, qraw, loc_sem.at[9])
    load_first = pltpu.make_async_copy(prefix.at[0, 0], stage.at[0, 0], loc_sem.at[0])
    load_first.start()
    load_q.start()
    barrier = pltpu.get_barrier_semaphore()
    line = (z + 2) % 8

    def mate(k):
        return (line // 4 * 4 + (line + k) % 4 + 6) % 8

    peers = [other, at(head, 1 - yl, z, c)]
    for k in range(1, 8):
        peers.append(at((head + k) % 8, yl, z, c))
    for k in range(1, 4):
        peers.append(at(head, yl, zh * 4 + (zl + k) % 4, c))
        peers.append(at(head, 1 - yl, zh * 4 + (zl + k) % 4, c))
    for k in range(2):
        peers.append(at(head, yl, (line // 4 * 4 + (line % 4 // 2 * 2 + 2 + k) % 4 + 6) % 8, c))
    for dev in peers:
        pl.semaphore_signal(barrier, inc=1, device_id=dev, device_id_type=MESH)

    order = ((0, 0), (1, 0), (0, 1), (1, 1))
    loads = {(l, k): pltpu.make_async_copy(prefix.at[l, k], stage.at[l, k], loc_sem.at[l * 2 + k])
             for l, k in order[1:]}
    owns = {(l, k): pltpu.make_async_copy(
        prefix.at[l, k, :, pl.ds(pl.multiple_of(part * POS, POS), POS)],
        kown.at[l, k, part], loc_sem.at[4 + l * 2 + k]) for l, k in order}
    load_suf = pltpu.make_async_copy(suffix, suf, loc_sem.at[8])
    load_len = pltpu.make_async_copy(lengths_in, lengths, loc_sem.at[10])
    load_slot = pltpu.make_async_copy(slot_in, slot, loc_sem.at[11])
    load_suf.start()
    load_len.start()
    load_slot.start()

    for l, k in order:
        if (l, k) != (0, 0):
            loads[l, k].start()
        owns[l, k].start()

    load_q.wait()
    q32 = qraw[...].astype(f32)
    for h in range(KVH):
        rows = [q32[l:l + 1, (h * GROUP + g) * HD:(h * GROUP + g + 1) * HD]
                for l in range(2) for g in range(GROUP)]
        qmsg[h] = jnp.concatenate(rows, axis=0).astype(bf16)
    pl.semaphore_wait(barrier, len(peers))

    for k in range(1, 8):
        to = (head + k) % 8
        remote(qmsg.at[to], qa.at[head], a_sem.at[0], a_sem.at[1], at(to, yl, z, c)).start()
    qa[head] = qmsg[head]

    def kv_send(l, k, steps, half=None):
        for dz, dy in steps:
            yl_to, zl_to = (yl + dy) % 2, (zl + dz) % 4
            to = yl_to * 4 + zl_to
            if half is None:
                start, size, dst, r = 0, POS, kown.at[l, k, part], kv_r.at[l * 2 + k]
            else:
                start, size = half * HALF, HALF
                dst = kown.at[l, k, part, :, start:start + HALF]
                r = v1_r.at[part] if half else kv_r.at[l * 2 + k]
            remote(
                stage.at[l, k, :, pl.ds(pl.multiple_of(to * POS + start, HALF), size)],
                dst, kv_s.at[l * 2 + k], r, at(head, yl_to, zh * 4 + zl_to, c)).start()

    def kv_wait(l, k):
        owns[l, k].wait()
        remote(kown.at[l, k, 0:7], kown.at[l, k, 0:7], kv_s.at[0], kv_r.at[l * 2 + k]).wait_recv()

    def forward(l, k):
        return remote(kown.at[l, k], koth.at[l, k], f_s.at[l * 2 + k], f_r.at[l * 2 + k])

    full = [(2, 0), (2, 1), (1, 0), (1, 1), (3, 0), (3, 1), (0, 1)]

    load_first.wait()
    kv_send(0, 0, [(2, 0), (2, 1), (0, 1), (1, 0)])

    load_suf.wait()
    load_len.wait()
    load_slot.wait()
    count = lengths[slot[0]]
    row = lax.broadcasted_iota(jnp.int32, (8, HD), 0)
    lane = lax.broadcasted_iota(jnp.int32, (8, HD), 1)
    valid = lane < count

    def suffix_head(h):
        cols = slice(h * HD, (h + 1) * HD)
        q = qmsg[h]
        s0 = dot(q, suf[0, 0, 0, :, cols], NT)
        s1 = dot(q, suf[1, 0, 0, :, cols], NT)
        s = jnp.where(valid, jnp.where(row < GROUP, s0, s1) * SCALE2, NEG)
        top = jnp.max(s, axis=1, keepdims=True)
        w = jnp.where(valid, jnp.exp2(s - top), 0.0).astype(bf16)
        den = jnp.sum(w.astype(f32), axis=1, keepdims=True)
        n0 = dot(w, suf[0, 0, 1, :, cols], NN)
        n1 = dot(w, suf[1, 0, 1, :, cols], NN)
        sbuf_o[h] = jnp.where(row < GROUP, n0, n1) / den
        sbuf_l[h] = jnp.broadcast_to(top + jnp.log2(den), (8, HD))

    def suffix_part():
        for h in range(KVH):
            suffix_head(h)

    suffix_part()

    def a_wait():
        remote(qa.at[0:7], qa.at[0:7], a_sem.at[0], a_sem.at[1]).wait_recv()

    a_wait()
    low = row < GROUP

    def regroup(a, b):
        return (jnp.where(low, a, pltpu.roll(b, GROUP, 0)), jnp.where(low, pltpu.roll(a, GROUP, 0), b))

    pairs = [regroup(qa[2 * j].astype(f32), qa[2 * j + 1].astype(f32)) for j in range(4)]
    qall[z, yl] = jnp.concatenate([p[l] for l in range(2) for p in pairs], axis=0).astype(bf16)
    mirror = zh * 4 + 3 - zl

    def b_send(block, z_to, r):
        remote(qall.at[block, yl], qall.at[block, yl], b_sem.at[0], r, at(head, yl, z_to, c)).start()

    def y_send(z_of):
        block = qall.at[z_of, yl]
        remote(block, block, y_sem.at[0], y_sem.at[1], at(head, 1 - yl, z, c)).start()

    b_send(z, mirror, b_sem.at[2])
    for k in (2, 1, 3):
        b_send(z, mate(k), b_sem.at[1])
    y_send(z)
    loads[1, 0].wait()
    kv_send(0, 0, [(1, 1), (3, 0), (3, 1)])
    kv_send(1, 0, [(2, 0)])

    def m_wait():
        remote(qall.at[mirror, yl], qall.at[mirror, yl], b_sem.at[0], b_sem.at[2]).wait_recv()

    m_wait()
    for k in (2, 1, 3):
        b_send(mirror, mate(k), b_sem.at[3])
    y_send(mirror)
    loads[0, 1].wait()
    kv_send(1, 0, full[1:])
    kv_send(0, 1, full[:2])
    kv_wait(0, 0)
    forward(0, 0).start()

    def b_wait(r):
        remote(qall.at[0:3, 0], qall.at[0:3, 0], b_sem.at[0], b_sem.at[r]).wait_recv()

    def y_wait():
        whole = qall.at[:, 1 - yl]
        remote(whole, whole, y_sem.at[0], y_sem.at[1]).wait_recv()

    b_wait(1)
    for k in range(1, 4):
        y_send(mate(k))
    kv_send(0, 1, full[2:5])
    b_wait(3)
    for k in range(1, 4):
        y_send(mate(k) // 4 * 4 + 3 - mate(k) % 4)
    kv_send(0, 1, full[5:])
    loads[1, 1].wait()

    def weights(l):
        forward(l, 0).wait_recv()
        r64 = lax.broadcasted_iota(jnp.int32, (2, 64, HD), 1)
        c64 = lax.broadcasted_iota(jnp.int32, (2, 64, HD), 2)

        def rows(i, carry):
            q = qall[pl.ds(i * 2, 2), :, l * 32:(l + 1) * 32, :].reshape(128, HD)
            at_rows = pl.ds(pl.multiple_of(i * 128, 128), 128)
            sa = dot(q, kown[l, 0].reshape(HD, POS), NN) * SCALE2
            sb = dot(q, koth[l, 0].reshape(HD, POS), NN) * SCALE2
            top = jnp.maximum(jnp.max(sa, axis=1, keepdims=True), jnp.max(sb, axis=1, keepdims=True))
            wa = jnp.exp2(sa - top).astype(bf16)
            wb = jnp.exp2(sb - top).astype(bf16)
            den = jnp.sum(wa.astype(f32) + wb.astype(f32), axis=1, keepdims=True)
            wbuf[l, 0, at_rows, :] = wa
            wbuf[l, 1, at_rows, :] = wb
            rden[l, at_rows, :] = jnp.broadcast_to(1.0 / den, (128, HD))
            big = jnp.broadcast_to(top + jnp.log2(den), (128, HD)).reshape(2, 64, HD)
            line = jnp.sum(jnp.where(c64 == r64 + l * 64, big, 0.0), axis=1, keepdims=True)
            if l == 0:
                lsend[pl.ds(i * 2, 2)] = line
            else:
                lsend[pl.ds(i * 2, 2)] = lsend[pl.ds(i * 2, 2)] + line
            return carry

        lax.fori_loop(0, 4, rows, 0, unroll=True)

    z_at = [(z + d) % 8 for d in range(8)]
    x_at = [(x + d) % 4 for d in range(4)]
    y_at = [(y + d) % 4 for d in range(4)]

    def partials(l, offsets):
        for dz, dx, dy in offsets:
            z_to, x_to, y_to = z_at[dz], x_at[dx], y_at[dy]
            dev = ((x_to * 4 + y_to) * 4 + z_to % 4, z_to // 4 * 2 + c)
            remote(osend.at[l, z_to * 16 + y_to % 2 * 8 + x_to * 2 + y_to // 2],
                   orecv.at[l, spot * 8 + z], c_s.at[l], c_r.at[l], dev).start()

    def store_partials(l, o):
        osend.at[l].reshape(512, HD)[...] = o.astype(bf16)
        orecv[l, spot * 8 + z] = osend[l, z * 16 + yl * 8 + head]

    def values_own(l):
        oacc[l] = dot(wbuf[l, 0], kown[l, 1].reshape(HD, POS), NT)

    def values_other(l):
        forward(l, 1).wait_recv()
        store_partials(l, (oacc[l] + dot(wbuf[l, 1], koth[l, 1].reshape(HD, POS), NT)) * rden[l])

    def sources():
        ls = jnp.concatenate([lsend[...].reshape(8, HD), jnp.full((120, HD), NEG, f32)], axis=0).T
        for half in range(2):
            for j in range(4):
                base = half * 32 + j * 8
                even, odd = regroup(ls[base:base + 8], ls[64 + base:72 + base])
                gsend[4 * j + half] = even
                gsend[4 * j + 2 + half] = odd
        for k in range(1, 16):
            to = (spot + k) % 16
            remote(gsend.at[to], grecv.at[spot], g_sem.at[0], g_sem.at[1],
                   at(to // 2, to % 2, z, c)).start()
        grecv[spot] = gsend[spot]

    def columns():
        remote(grecv.at[0:15], grecv.at[0:15], g_sem.at[0], g_sem.at[1]).wait_recv()
        hsend[...] = grecv[...].reshape(128, HD).T[:8].reshape(8, 1, HD)
        for k in (4, 3, 5, 2, 6, 1, 7):
            to = (z + k) % 8
            remote(hsend.at[to], lrecv.at[z], l_sem.at[0], l_sem.at[1], at(head, yl, to, c)).start()
        lrecv[z] = hsend[z]

    kv_wait(1, 0)
    forward(1, 0).start()
    kv_send(1, 1, full, 0)
    y_wait()
    weights(0)
    kv_send(1, 1, full, 1)
    weights(1)
    sources()
    kv_wait(0, 1)
    forward(0, 1).start()
    values_own(0)

    first, second = slice(0, HALF), slice(HALF, POS)

    def last_first():
        owns[1, 1].wait()
        piece = kown.at[1, 1, 0:7, :, first]
        remote(piece, piece, kv_s.at[0], kv_r.at[3]).wait_recv()

    def last_copy():
        return remote(kown.at[1, 1, :, :, first], koth.at[1, 1, :, :, first], f_s.at[4], f_r.at[4])

    def last_dot(which, ref, span):
        return dot(wbuf[1, which, :, span], ref[1, 1, :, :, span].reshape(HD, HALF), NT)

    def values_first():
        oacc[1] = last_dot(0, kown, first)

    def last_pieces():
        own = kown.at[1, 1, part, :, second]
        remote(own, koth.at[1, 1, part, :, second], f_s.at[3], f_r.at[3]).start()
        for dz, dy in full:
            src = (yl + dy) % 2 * 4 + (zl + 4 - dz) % 4
            piece = kown.at[1, 1, src, :, second]
            remote(piece, piece, kv_s.at[0], v1_r.at[src]).wait_recv()
            remote(piece, koth.at[1, 1, src, :, second], f_s.at[3], f_r.at[3]).start()

    def values_second():
        oacc[1] = oacc[1] + last_dot(0, kown, second)
        last_copy().wait_recv()
        oacc[1] = oacc[1] + last_dot(1, koth, first)
        columns()
        whole = koth.at[1, 1, :, :, second]
        remote(whole, whole, f_s.at[3], f_r.at[3]).wait_recv()
        store_partials(1, (oacc[1] + last_dot(1, koth, second)) * rden[1])

    values_other(0)
    partials(0, FAR)
    last_first()
    last_copy().start()
    values_first()
    last_pieces()
    values_second()
    partials(1, FAR)
    partials(1, NEAR)
    partials(0, NEAR)

    def shares():
        remote(lrecv.at[0:7], lrecv.at[0:7], l_sem.at[0], l_sem.at[1]).wait_recv()
        ls = jnp.concatenate([lrecv[...].reshape(8, HD), jnp.full((120, HD), NEG, f32)], axis=0).T
        lfin[...] = ls.reshape(16, 8, HD)

        def one_head(h, carry):
            la, lb, lc = lfin[2 * h], lfin[2 * h + 1], sbuf_l[h]
            top = jnp.max(jnp.maximum(jnp.maximum(la, lb), lc), axis=1, keepdims=True)
            a, b, s = jnp.exp2(la - top), jnp.exp2(lb - top), jnp.exp2(lc - top)
            den = jnp.sum(a + b, axis=1, keepdims=True) + s
            sbuf_o[h] = s / den * sbuf_o[h]
            for half, w in enumerate((a / den, b / den)):
                for j in range(4):
                    pair = [jnp.broadcast_to(w[:, k:k + 1], (8, HD)) for k in (2 * j, 2 * j + 1)]
                    for l, tile in enumerate(regroup(*pair)):
                        share[l, 2 * h + half, j] = tile
            return carry

        lax.fori_loop(0, KVH, one_head, 0)

    def finish(l):
        remote(orecv.at[l, 0:127], orecv.at[l, 0:127], c_s.at[l], c_r.at[l]).wait_recv()
        got = orecv.at[l].reshape(512, HD)[...].astype(f32).reshape(KVH, 8, 8, HD)
        return jnp.sum(got * share[l].reshape(KVH, 8, 8, HD), axis=1)

    shares()
    o0 = finish(0)
    o1 = finish(1)
    for h in range(KVH):
        first_half, last_half = regroup(o0[h], o1[h])
        both = first_half + last_half + sbuf_o[h]
        for g in range(GROUP):
            pair = jnp.concatenate([both[g:g + 1], both[GROUP + g:GROUP + g + 1]], axis=0)
            out[:, (h * GROUP + g) * HD:(h * GROUP + g + 1) * HD] = pair.astype(bf16)

    remote(qa.at[0:7], qa.at[0:7], a_sem.at[0], a_sem.at[1]).wait_send()
    remote(qall.at[0:7, 0], qall.at[0:7, 0], b_sem.at[0], b_sem.at[1]).wait_send()
    remote(qall.at[:, yl], qall.at[:, yl], y_sem.at[0], y_sem.at[1]).wait_send()
    last_copy().wait_send()
    remote(kown.at[1, 1, :, :, second], koth.at[1, 1, :, :, second], f_s.at[3], f_r.at[3]).wait_send()
    remote(lrecv.at[0:7], lrecv.at[0:7], l_sem.at[0], l_sem.at[1]).wait_send()
    remote(grecv.at[0:15], grecv.at[0:15], g_sem.at[0], g_sem.at[1]).wait_send()
    for l in range(2):
        for k in range(2):
            remote(kown.at[l, k, 0:7], kown.at[l, k, 0:7], kv_s.at[l * 2 + k], kv_r.at[0]).wait_send()
            if (l, k) != (1, 1):
                forward(l, k).wait_send()
        remote(orecv.at[l, 0:127], orecv.at[l, 0:127], c_s.at[l], c_r.at[l]).wait_send()


def body(prefix_cache, queries, suffix_cache, suffix_lengths, slot_request):
    bf, f32 = jnp.bfloat16, jnp.float32
    dma = pltpu.SemaphoreType.DMA
    any_space = pl.BlockSpec(memory_space=pl.ANY)
    out = pl.pallas_call(
        kernel,
        out_shape=pltpu.VMEM((2, QH * HD), bf),
        in_specs=[
            any_space,
            any_space,
            any_space,
            any_space,
            any_space,
        ],
        out_specs=pl.BlockSpec(memory_space=pltpu.VMEM),
        scratch_shapes=[
            pltpu.SMEM((256,), jnp.int32),
            pltpu.SMEM((1,), jnp.int32),
            pltpu.VMEM((2, 2, 16, 8192), bf),
            pltpu.VMEM((2, 2, 8, 16, POS), bf),
            pltpu.VMEM((2, 2, 8, 16, POS), bf),
            pltpu.VMEM((2, 1, 2, SUF, KVH * HD), bf),
            pltpu.VMEM((2, QH * HD), bf),
            pltpu.VMEM((8, 8, HD), bf),
            pltpu.VMEM((8, 8, HD), bf),
            pltpu.VMEM((8, 2, 64, HD), bf),
            pltpu.VMEM((2, 2, 512, POS), bf),
            pltpu.VMEM((2, 512, HD), f32),
            pltpu.VMEM((2, 512, HD), f32),
            pltpu.VMEM((KVH, 8, HD), f32),
            pltpu.VMEM((KVH, 8, HD), f32),
            pltpu.VMEM((2, 128, GROUP, HD), bf),
            pltpu.VMEM((2, 128, GROUP, HD), bf),
            pltpu.VMEM((8, 1, HD), f32),
            pltpu.VMEM((8, 1, HD), f32),
            pltpu.VMEM((8, 1, HD), f32),
            pltpu.VMEM((16, 8, HD), f32),
            pltpu.VMEM((16, 8, HD), f32),
            pltpu.VMEM((16, 8, HD), f32),
            pltpu.VMEM((2, 16, 4, 8, HD), f32),
            dma((12,)),
            dma((2,)), dma((4,)), dma((2,)),
            dma((4,)), dma((4,)), dma((8,)),
            dma((5,)), dma((5,)),
            dma((2,)), dma((2,)),
            dma((2,)), dma((2,)),
        ],
        compiler_params=pltpu.CompilerParams(collective_id=0, has_side_effects=True),
        name="attend",
    )(prefix_cache, queries.reshape(2, QH * HD), suffix_cache, suffix_lengths, slot_request)
    return out.reshape(2, 1, QH * HD)


def solution(mesh):
    in_specs = (
        P(None, None, "seq", "rep"),
        P(None, ("seq", "rep"), None),
        P(None, ("seq", "rep"), None, None, None),
        P(),
        P(("seq", "rep")),
    )
    out_specs = P(None, ("seq", "rep"), None)
    return jax.shard_map(body, mesh=mesh, in_specs=in_specs, out_specs=out_specs, check_vma=False)
```

```python
import math

import jax
import jax.numpy as jnp
from jax import lax
from jax.experimental import pallas as pl
from jax.experimental.pallas import tpu as pltpu
from jax.sharding import PartitionSpec as P

QH = 32
KVH = 8
HD = 128
SUF = 128
GROUP = 4
NEG = -1e30
SCALE2 = HD ** -0.5 * math.log2(math.e)
POS = 1024
HALF = POS // 2
NT = (((1,), (1,)), ((), ()))
NN = (((1,), (0,)), ((), ()))
MESH = pl.DeviceIdType.MESH
OFFSETS = sorted(
    [(dz, dx, dy) for dz in range(8) for dx in range(4) for dy in range(4) if dz + dx + dy],
    key=lambda o: -(min(o[0], 8 - o[0]) + min(o[1], 4 - o[1]) + min(o[2], 4 - o[2])))
FAR, NEAR = OFFSETS[:64], OFFSETS[64:]


def dot(a, b, dims):
    return lax.dot_general(a, b, dims, preferred_element_type=jnp.float32)


def kernel(
    prefix, queries, suffix, lengths_in, slot_in, out,
    lengths, slot, stage, kown, koth, suf, qraw, qmsg, qa, qall, wbuf, rden, oacc, sbuf_o, sbuf_l,
    osend, orecv, lsend, hsend, lrecv, gsend, grecv, lfin, share,
    loc_sem, a_sem, b_sem, y_sem, kv_s, kv_r, v1_r, f_s, f_r, c_s, c_r, l_sem, g_sem,
):
    f32, bf16 = jnp.float32, jnp.bfloat16
    seq = lax.axis_index("seq")
    rep = lax.axis_index("rep")
    x, y, zl = seq // 16, (seq // 4) % 4, seq % 4
    yh, yl = y // 2, y % 2
    zh, c = rep // 2, rep % 2
    z = zh * 4 + zl
    head = x * 2 + yh
    part = yl * 4 + zl
    spot = head * 2 + yl

    def at(head_to, yl_to, z_to, c_to):
        x_to, yh_to = head_to // 2, head_to % 2
        return ((x_to * 4 + yh_to * 2 + yl_to) * 4 + z_to % 4, (z_to // 4) * 2 + c_to)

    other = at(head, yl, z, 1 - c)

    def remote(src, dst, s, r, dev=other):
        return pltpu.make_async_remote_copy(
            src_ref=src, dst_ref=dst, send_sem=s, recv_sem=r, device_id=dev, device_id_type=MESH)

    load_q = pltpu.make_async_copy(queries, qraw, loc_sem.at[9])
    load_first = pltpu.make_async_copy(prefix.at[0, 0], stage.at[0, 0], loc_sem.at[0])
    load_first.start()
    load_q.start()
    barrier = pltpu.get_barrier_semaphore()
    line = (z + 2) % 8

    def mate(k):
        return (line // 4 * 4 + (line + k) % 4 + 6) % 8

    peers = [other, at(head, 1 - yl, z, c)]
    for k in range(1, 8):
        peers.append(at((head + k) % 8, yl, z, c))
    for k in range(1, 4):
        peers.append(at(head, yl, zh * 4 + (zl + k) % 4, c))
        peers.append(at(head, 1 - yl, zh * 4 + (zl + k) % 4, c))
    for k in range(2):
        peers.append(at(head, yl, (line // 4 * 4 + (line % 4 // 2 * 2 + 2 + k) % 4 + 6) % 8, c))
    for dev in peers:
        pl.semaphore_signal(barrier, inc=1, device_id=dev, device_id_type=MESH)

    order = ((0, 0), (1, 0), (0, 1), (1, 1))
    loads = {(l, k): pltpu.make_async_copy(prefix.at[l, k], stage.at[l, k], loc_sem.at[l * 2 + k])
             for l, k in order[1:]}
    owns = {(l, k): pltpu.make_async_copy(
        prefix.at[l, k, :, pl.ds(pl.multiple_of(part * POS, POS), POS)],
        kown.at[l, k, part], loc_sem.at[4 + l * 2 + k]) for l, k in order}
    load_suf = pltpu.make_async_copy(suffix, suf, loc_sem.at[8])
    load_len = pltpu.make_async_copy(lengths_in, lengths, loc_sem.at[10])
    load_slot = pltpu.make_async_copy(slot_in, slot, loc_sem.at[11])
    load_suf.start()
    load_len.start()
    load_slot.start()

    for l, k in order:
        if (l, k) != (0, 0):
            loads[l, k].start()
        owns[l, k].start()

    load_q.wait()
    q32 = qraw[...].astype(f32)
    for h in range(KVH):
        rows = [q32[l:l + 1, (h * GROUP + g) * HD:(h * GROUP + g + 1) * HD]
                for l in range(2) for g in range(GROUP)]
        qmsg[h] = jnp.concatenate(rows, axis=0).astype(bf16)
    pl.semaphore_wait(barrier, len(peers))

    for k in range(1, 8):
        to = (head + k) % 8
        remote(qmsg.at[to], qa.at[head], a_sem.at[0], a_sem.at[1], at(to, yl, z, c)).start()
    qa[head] = qmsg[head]

    def kv_send(l, k, steps, half=None):
        for dz, dy in steps:
            yl_to, zl_to = (yl + dy) % 2, (zl + dz) % 4
            to = yl_to * 4 + zl_to
            if half is None:
                start, size, dst, r = 0, POS, kown.at[l, k, part], kv_r.at[l * 2 + k]
            else:
                start, size = half * HALF, HALF
                dst = kown.at[l, k, part, :, start:start + HALF]
                r = v1_r.at[part] if half else kv_r.at[l * 2 + k]
            remote(
                stage.at[l, k, :, pl.ds(pl.multiple_of(to * POS + start, HALF), size)],
                dst, kv_s.at[l * 2 + k], r, at(head, yl_to, zh * 4 + zl_to, c)).start()

    def kv_wait(l, k):
        owns[l, k].wait()
        remote(kown.at[l, k, 0:7], kown.at[l, k, 0:7], kv_s.at[0], kv_r.at[l * 2 + k]).wait_recv()

    def forward(l, k):
        return remote(kown.at[l, k], koth.at[l, k], f_s.at[l * 2 + k], f_r.at[l * 2 + k])

    to_mirror, to_next = 3 - 2 * (zl % 2), 1 + 2 * (zl % 2)
    full = [(to_mirror, 0), (to_mirror, 1), (2, 0), (2, 1), (to_next, 0), (to_next, 1), (0, 1)]

    load_first.wait()
    kv_send(0, 0, full[:3] + full[6:])

    load_suf.wait()
    load_len.wait()
    load_slot.wait()
    count = lengths[slot[0]]
    row = lax.broadcasted_iota(jnp.int32, (8, HD), 0)
    lane = lax.broadcasted_iota(jnp.int32, (8, HD), 1)
    valid = lane < count

    def suffix_head(h):
        cols = slice(h * HD, (h + 1) * HD)
        q = qmsg[h]
        s0 = dot(q, suf[0, 0, 0, :, cols], NT)
        s1 = dot(q, suf[1, 0, 0, :, cols], NT)
        s = jnp.where(valid, jnp.where(row < GROUP, s0, s1) * SCALE2, NEG)
        top = jnp.max(s, axis=1, keepdims=True)
        w = jnp.where(valid, jnp.exp2(s - top), 0.0).astype(bf16)
        den = jnp.sum(w.astype(f32), axis=1, keepdims=True)
        n0 = dot(w, suf[0, 0, 1, :, cols], NN)
        n1 = dot(w, suf[1, 0, 1, :, cols], NN)
        sbuf_o[h] = jnp.where(row < GROUP, n0, n1) / den
        sbuf_l[h] = jnp.broadcast_to(top + jnp.log2(den), (8, HD))

    def suffix_part():
        for h in range(KVH):
            suffix_head(h)

    suffix_part()

    def a_wait():
        remote(qa.at[0:7], qa.at[0:7], a_sem.at[0], a_sem.at[1]).wait_recv()

    a_wait()
    low = row < GROUP

    def regroup(a, b):
        return (jnp.where(low, a, pltpu.roll(b, GROUP, 0)), jnp.where(low, pltpu.roll(a, GROUP, 0), b))

    pairs = [regroup(qa[2 * j].astype(f32), qa[2 * j + 1].astype(f32)) for j in range(4)]
    qall[z, yl] = jnp.concatenate([p[l] for l in range(2) for p in pairs], axis=0).astype(bf16)
    mirror = zh * 4 + 3 - zl

    def b_send(block, z_to, r):
        remote(qall.at[block, yl], qall.at[block, yl], b_sem.at[0], r, at(head, yl, z_to, c)).start()

    def y_send(z_of):
        block = qall.at[z_of, yl]
        remote(block, block, y_sem.at[0], y_sem.at[1], at(head, 1 - yl, z, c)).start()

    b_send(z, mirror, b_sem.at[2])
    for k in (2, 1, 3):
        b_send(z, mate(k), b_sem.at[1])
    y_send(z)
    loads[1, 0].wait()
    kv_send(0, 0, full[3:6])
    kv_send(1, 0, full[:1])

    def m_wait():
        remote(qall.at[mirror, yl], qall.at[mirror, yl], b_sem.at[0], b_sem.at[2]).wait_recv()

    m_wait()
    for k in (2, 1, 3):
        b_send(mirror, mate(k), b_sem.at[3])
    y_send(mirror)
    loads[0, 1].wait()
    kv_send(1, 0, full[1:])
    kv_send(0, 1, full[:2])
    kv_wait(0, 0)
    forward(0, 0).start()

    def b_wait(r):
        remote(qall.at[0:3, 0], qall.at[0:3, 0], b_sem.at[0], b_sem.at[r]).wait_recv()

    def y_wait():
        whole = qall.at[:, 1 - yl]
        remote(whole, whole, y_sem.at[0], y_sem.at[1]).wait_recv()

    b_wait(1)
    for k in range(1, 4):
        y_send(mate(k))
    kv_send(0, 1, full[2:5])
    b_wait(3)
    for k in range(1, 4):
        y_send(mate(k) // 4 * 4 + 3 - mate(k) % 4)
    kv_send(0, 1, full[5:])
    loads[1, 1].wait()

    def weights(l):
        forward(l, 0).wait_recv()
        r64 = lax.broadcasted_iota(jnp.int32, (2, 64, HD), 1)
        c64 = lax.broadcasted_iota(jnp.int32, (2, 64, HD), 2)

        def rows(i, carry):
            q = qall[pl.ds(i * 2, 2), :, l * 32:(l + 1) * 32, :].reshape(128, HD)
            at_rows = pl.ds(pl.multiple_of(i * 128, 128), 128)
            sa = dot(q, kown[l, 0].reshape(HD, POS), NN) * SCALE2
            sb = dot(q, koth[l, 0].reshape(HD, POS), NN) * SCALE2
            top = jnp.maximum(jnp.max(sa, axis=1, keepdims=True), jnp.max(sb, axis=1, keepdims=True))
            wa = jnp.exp2(sa - top).astype(bf16)
            wb = jnp.exp2(sb - top).astype(bf16)
            den = jnp.sum(wa.astype(f32) + wb.astype(f32), axis=1, keepdims=True)
            wbuf[l, 0, at_rows, :] = wa
            wbuf[l, 1, at_rows, :] = wb
            rden[l, at_rows, :] = jnp.broadcast_to(1.0 / den, (128, HD))
            big = jnp.broadcast_to(top + jnp.log2(den), (128, HD)).reshape(2, 64, HD)
            line = jnp.sum(jnp.where(c64 == r64 + l * 64, big, 0.0), axis=1, keepdims=True)
            if l == 0:
                lsend[pl.ds(i * 2, 2)] = line
            else:
                lsend[pl.ds(i * 2, 2)] = lsend[pl.ds(i * 2, 2)] + line
            return carry

        lax.fori_loop(0, 4, rows, 0, unroll=True)

    z_at = [(z + d) % 8 for d in range(8)]
    x_at = [(x + d) % 4 for d in range(4)]
    y_at = [(y + d) % 4 for d in range(4)]

    def partials(l, offsets):
        for dz, dx, dy in offsets:
            z_to, x_to, y_to = z_at[dz], x_at[dx], y_at[dy]
            dev = ((x_to * 4 + y_to) * 4 + z_to % 4, z_to // 4 * 2 + c)
            remote(osend.at[l, z_to * 16 + y_to % 2 * 8 + x_to * 2 + y_to // 2],
                   orecv.at[l, spot * 8 + z], c_s.at[l], c_r.at[l], dev).start()

    def store_partials(l, o):
        osend.at[l].reshape(512, HD)[...] = o.astype(bf16)
        orecv[l, spot * 8 + z] = osend[l, z * 16 + yl * 8 + head]

    def values_own(l):
        oacc[l] = dot(wbuf[l, 0], kown[l, 1].reshape(HD, POS), NT)

    def values_other(l):
        forward(l, 1).wait_recv()
        store_partials(l, (oacc[l] + dot(wbuf[l, 1], koth[l, 1].reshape(HD, POS), NT)) * rden[l])

    def sources():
        ls = jnp.concatenate([lsend[...].reshape(8, HD), jnp.full((120, HD), NEG, f32)], axis=0).T
        for half in range(2):
            for j in range(4):
                base = half * 32 + j * 8
                even, odd = regroup(ls[base:base + 8], ls[64 + base:72 + base])
                gsend[4 * j + half] = even
                gsend[4 * j + 2 + half] = odd
        for k in range(1, 16):
            to = (spot + k) % 16
            remote(gsend.at[to], grecv.at[spot], g_sem.at[0], g_sem.at[1],
                   at(to // 2, to % 2, z, c)).start()
        grecv[spot] = gsend[spot]

    def columns():
        remote(grecv.at[0:15], grecv.at[0:15], g_sem.at[0], g_sem.at[1]).wait_recv()
        hsend[...] = grecv[...].reshape(128, HD).T[:8].reshape(8, 1, HD)
        for k in (4, 3, 5, 2, 6, 1, 7):
            to = (z + k) % 8
            remote(hsend.at[to], lrecv.at[z], l_sem.at[0], l_sem.at[1], at(head, yl, to, c)).start()
        lrecv[z] = hsend[z]

    kv_wait(1, 0)
    forward(1, 0).start()
    kv_send(1, 1, full, 0)
    y_wait()
    weights(0)
    kv_send(1, 1, full, 1)
    weights(1)
    sources()
    kv_wait(0, 1)
    forward(0, 1).start()
    values_own(0)

    first, second = slice(0, HALF), slice(HALF, POS)

    def last_first():
        owns[1, 1].wait()
        piece = kown.at[1, 1, 0:7, :, first]
        remote(piece, piece, kv_s.at[0], kv_r.at[3]).wait_recv()

    def last_copy():
        return remote(kown.at[1, 1, :, :, first], koth.at[1, 1, :, :, first], f_s.at[4], f_r.at[4])

    def last_dot(which, ref, span):
        return dot(wbuf[1, which, :, span], ref[1, 1, :, :, span].reshape(HD, HALF), NT)

    def values_first():
        oacc[1] = last_dot(0, kown, first)

    def last_pieces():
        own = kown.at[1, 1, part, :, second]
        remote(own, koth.at[1, 1, part, :, second], f_s.at[3], f_r.at[3]).start()
        for dz, dy in full:
            src = (yl + dy) % 2 * 4 + (zl + dz) % 4
            piece = kown.at[1, 1, src, :, second]
            remote(piece, piece, kv_s.at[0], v1_r.at[src]).wait_recv()
            remote(piece, koth.at[1, 1, src, :, second], f_s.at[3], f_r.at[3]).start()

    def values_second():
        oacc[1] = oacc[1] + last_dot(0, kown, second)
        last_copy().wait_recv()
        oacc[1] = oacc[1] + last_dot(1, koth, first)
        columns()
        whole = koth.at[1, 1, :, :, second]
        remote(whole, whole, f_s.at[3], f_r.at[3]).wait_recv()
        store_partials(1, (oacc[1] + last_dot(1, koth, second)) * rden[1])

    values_other(0)
    partials(0, FAR)
    last_first()
    last_copy().start()
    values_first()
    last_pieces()
    values_second()
    partials(1, FAR)
    partials(1, NEAR)
    partials(0, NEAR)

    def shares():
        remote(lrecv.at[0:7], lrecv.at[0:7], l_sem.at[0], l_sem.at[1]).wait_recv()
        ls = jnp.concatenate([lrecv[...].reshape(8, HD), jnp.full((120, HD), NEG, f32)], axis=0).T
        lfin[...] = ls.reshape(16, 8, HD)

        def one_head(h, carry):
            la, lb, lc = lfin[2 * h], lfin[2 * h + 1], sbuf_l[h]
            top = jnp.max(jnp.maximum(jnp.maximum(la, lb), lc), axis=1, keepdims=True)
            a, b, s = jnp.exp2(la - top), jnp.exp2(lb - top), jnp.exp2(lc - top)
            den = jnp.sum(a + b, axis=1, keepdims=True) + s
            sbuf_o[h] = s / den * sbuf_o[h]
            for half, w in enumerate((a / den, b / den)):
                for j in range(4):
                    pair = [jnp.broadcast_to(w[:, k:k + 1], (8, HD)) for k in (2 * j, 2 * j + 1)]
                    for l, tile in enumerate(regroup(*pair)):
                        share[l, 2 * h + half, j] = tile
            return carry

        lax.fori_loop(0, KVH, one_head, 0)

    def finish(l):
        remote(orecv.at[l, 0:127], orecv.at[l, 0:127], c_s.at[l], c_r.at[l]).wait_recv()
        got = orecv.at[l].reshape(512, HD)[...].astype(f32).reshape(KVH, 8, 8, HD)
        return jnp.sum(got * share[l].reshape(KVH, 8, 8, HD), axis=1)

    shares()
    o0 = finish(0)
    o1 = finish(1)
    for h in range(KVH):
        first_half, last_half = regroup(o0[h], o1[h])
        both = first_half + last_half + sbuf_o[h]
        for g in range(GROUP):
            pair = jnp.concatenate([both[g:g + 1], both[GROUP + g:GROUP + g + 1]], axis=0)
            out[:, (h * GROUP + g) * HD:(h * GROUP + g + 1) * HD] = pair.astype(bf16)

    remote(qa.at[0:7], qa.at[0:7], a_sem.at[0], a_sem.at[1]).wait_send()
    remote(qall.at[0:7, 0], qall.at[0:7, 0], b_sem.at[0], b_sem.at[1]).wait_send()
    remote(qall.at[:, yl], qall.at[:, yl], y_sem.at[0], y_sem.at[1]).wait_send()
    last_copy().wait_send()
    remote(kown.at[1, 1, :, :, second], koth.at[1, 1, :, :, second], f_s.at[3], f_r.at[3]).wait_send()
    remote(lrecv.at[0:7], lrecv.at[0:7], l_sem.at[0], l_sem.at[1]).wait_send()
    remote(grecv.at[0:15], grecv.at[0:15], g_sem.at[0], g_sem.at[1]).wait_send()
    for l in range(2):
        for k in range(2):
            remote(kown.at[l, k, 0:7], kown.at[l, k, 0:7], kv_s.at[l * 2 + k], kv_r.at[0]).wait_send()
            if (l, k) != (1, 1):
                forward(l, k).wait_send()
        remote(orecv.at[l, 0:127], orecv.at[l, 0:127], c_s.at[l], c_r.at[l]).wait_send()


def body(prefix_cache, queries, suffix_cache, suffix_lengths, slot_request):
    bf, f32 = jnp.bfloat16, jnp.float32
    dma = pltpu.SemaphoreType.DMA
    any_space = pl.BlockSpec(memory_space=pl.ANY)
    out = pl.pallas_call(
        kernel,
        out_shape=pltpu.VMEM((2, QH * HD), bf),
        in_specs=[
            any_space,
            any_space,
            any_space,
            any_space,
            any_space,
        ],
        out_specs=pl.BlockSpec(memory_space=pltpu.VMEM),
        scratch_shapes=[
            pltpu.SMEM((256,), jnp.int32),
            pltpu.SMEM((1,), jnp.int32),
            pltpu.VMEM((2, 2, 16, 8192), bf),
            pltpu.VMEM((2, 2, 8, 16, POS), bf),
            pltpu.VMEM((2, 2, 8, 16, POS), bf),
            pltpu.VMEM((2, 1, 2, SUF, KVH * HD), bf),
            pltpu.VMEM((2, QH * HD), bf),
            pltpu.VMEM((8, 8, HD), bf),
            pltpu.VMEM((8, 8, HD), bf),
            pltpu.VMEM((8, 2, 64, HD), bf),
            pltpu.VMEM((2, 2, 512, POS), bf),
            pltpu.VMEM((2, 512, HD), f32),
            pltpu.VMEM((2, 512, HD), f32),
            pltpu.VMEM((KVH, 8, HD), f32),
            pltpu.VMEM((KVH, 8, HD), f32),
            pltpu.VMEM((2, 128, GROUP, HD), bf),
            pltpu.VMEM((2, 128, GROUP, HD), bf),
            pltpu.VMEM((8, 1, HD), f32),
            pltpu.VMEM((8, 1, HD), f32),
            pltpu.VMEM((8, 1, HD), f32),
            pltpu.VMEM((16, 8, HD), f32),
            pltpu.VMEM((16, 8, HD), f32),
            pltpu.VMEM((16, 8, HD), f32),
            pltpu.VMEM((2, 16, 4, 8, HD), f32),
            dma((12,)),
            dma((2,)), dma((4,)), dma((2,)),
            dma((4,)), dma((4,)), dma((8,)),
            dma((5,)), dma((5,)),
            dma((2,)), dma((2,)),
            dma((2,)), dma((2,)),
        ],
        compiler_params=pltpu.CompilerParams(collective_id=0, has_side_effects=True),
        name="attend",
    )(prefix_cache, queries.reshape(2, QH * HD), suffix_cache, suffix_lengths, slot_request)
    return out.reshape(2, 1, QH * HD)


def solution(mesh):
    in_specs = (
        P(None, None, "seq", "rep"),
        P(None, ("seq", "rep"), None),
        P(None, ("seq", "rep"), None, None, None),
        P(),
        P(("seq", "rep")),
    )
    out_specs = P(None, ("seq", "rep"), None)
    return jax.shard_map(body, mesh=mesh, in_specs=in_specs, out_specs=out_specs, check_vma=False)
```

```python
import math

import jax
import jax.numpy as jnp
from jax import lax
from jax.experimental import pallas as pl
from jax.experimental.pallas import tpu as pltpu
from jax.sharding import PartitionSpec as P

QH = 32
KVH = 8
HD = 128
SUF = 128
GROUP = 4
NEG = -1e30
SCALE2 = HD ** -0.5 * math.log2(math.e)
POS = 1024
HALF = POS // 2
NT = (((1,), (1,)), ((), ()))
NN = (((1,), (0,)), ((), ()))
MESH = pl.DeviceIdType.MESH
OFFSETS = sorted(
    [(dz, dx, dy) for dz in range(8) for dx in range(4) for dy in range(4) if dz + dx + dy],
    key=lambda o: -(min(o[0], 8 - o[0]) + min(o[1], 4 - o[1]) + min(o[2], 4 - o[2])))
FAR, NEAR = OFFSETS[:64], OFFSETS[64:]


def dot(a, b, dims):
    return lax.dot_general(a, b, dims, preferred_element_type=jnp.float32)


def kernel(
    prefix, queries, suffix, lengths_in, slot_in, out,
    lengths, slot, stage, kown, koth, suf, qraw, qmsg, qa, qall, wbuf, rden, oacc, sbuf_o, sbuf_l,
    osend, orecv, lsend, hsend, lrecv, gsend, grecv, lfin, share,
    loc_sem, a_sem, b_sem, y_sem, kv_s, kv_r, v1_r, f_s, f_r, c_s, c_r, l_sem, g_sem,
):
    f32, bf16 = jnp.float32, jnp.bfloat16
    seq = lax.axis_index("seq")
    rep = lax.axis_index("rep")
    x, y, zl = seq // 16, (seq // 4) % 4, seq % 4
    yh, yl = y // 2, y % 2
    zh, c = rep // 2, rep % 2
    z = zh * 4 + zl
    head = x * 2 + yh
    part = yl * 4 + zl
    spot = head * 2 + yl

    def at(head_to, yl_to, z_to, c_to):
        x_to, yh_to = head_to // 2, head_to % 2
        return ((x_to * 4 + yh_to * 2 + yl_to) * 4 + z_to % 4, (z_to // 4) * 2 + c_to)

    other = at(head, yl, z, 1 - c)

    def remote(src, dst, s, r, dev=other):
        return pltpu.make_async_remote_copy(
            src_ref=src, dst_ref=dst, send_sem=s, recv_sem=r, device_id=dev, device_id_type=MESH)

    load_q = pltpu.make_async_copy(queries, qraw, loc_sem.at[9])
    load_first = pltpu.make_async_copy(prefix.at[0, 0], stage.at[0, 0], loc_sem.at[0])
    load_first.start()
    load_q.start()
    barrier = pltpu.get_barrier_semaphore()
    line = (z + 2) % 8

    def mate(k):
        return (line // 4 * 4 + (line + k) % 4 + 6) % 8

    peers = [other, at(head, 1 - yl, z, c)]
    for k in range(1, 8):
        peers.append(at((head + k) % 8, yl, z, c))
    for k in range(1, 4):
        peers.append(at(head, yl, zh * 4 + (zl + k) % 4, c))
        peers.append(at(head, 1 - yl, zh * 4 + (zl + k) % 4, c))
    for k in range(2):
        peers.append(at(head, yl, (line // 4 * 4 + (line % 4 // 2 * 2 + 2 + k) % 4 + 6) % 8, c))
    for dev in peers:
        pl.semaphore_signal(barrier, inc=1, device_id=dev, device_id_type=MESH)

    order = ((0, 0), (1, 0), (0, 1), (1, 1))
    loads = {(l, k): pltpu.make_async_copy(prefix.at[l, k], stage.at[l, k], loc_sem.at[l * 2 + k])
             for l, k in order[1:]}
    owns = {(l, k): pltpu.make_async_copy(
        prefix.at[l, k, :, pl.ds(pl.multiple_of(part * POS, POS), POS)],
        kown.at[l, k, part], loc_sem.at[4 + l * 2 + k]) for l, k in order}
    load_suf = pltpu.make_async_copy(suffix, suf, loc_sem.at[8])
    load_len = pltpu.make_async_copy(lengths_in, lengths, loc_sem.at[10])
    load_slot = pltpu.make_async_copy(slot_in, slot, loc_sem.at[11])
    load_suf.start()
    load_len.start()
    load_slot.start()

    for l, k in order:
        if (l, k) != (0, 0):
            loads[l, k].start()
        owns[l, k].start()

    load_q.wait()
    q32 = qraw[...].astype(f32)
    for h in range(KVH):
        rows = [q32[l:l + 1, (h * GROUP + g) * HD:(h * GROUP + g + 1) * HD]
                for l in range(2) for g in range(GROUP)]
        qmsg[h] = jnp.concatenate(rows, axis=0).astype(bf16)
    pl.semaphore_wait(barrier, len(peers))

    for k in range(1, 8):
        to = (head + k) % 8
        remote(qmsg.at[to], qa.at[head], a_sem.at[0], a_sem.at[1], at(to, yl, z, c)).start()
    qa[head] = qmsg[head]

    def kv_send(l, k, steps, half=None):
        for dz, dy in steps:
            yl_to, zl_to = (yl + dy) % 2, (zl + dz) % 4
            to = yl_to * 4 + zl_to
            if half is None:
                start, size, dst, r = 0, POS, kown.at[l, k, part], kv_r.at[l * 2 + k]
            else:
                start, size = half * HALF, HALF
                dst = kown.at[l, k, part, :, start:start + HALF]
                r = v1_r.at[part] if half else kv_r.at[l * 2 + k]
            remote(
                stage.at[l, k, :, pl.ds(pl.multiple_of(to * POS + start, HALF), size)],
                dst, kv_s.at[l * 2 + k], r, at(head, yl_to, zh * 4 + zl_to, c)).start()

    def kv_wait(l, k):
        owns[l, k].wait()
        remote(kown.at[l, k, 0:7], kown.at[l, k, 0:7], kv_s.at[0], kv_r.at[l * 2 + k]).wait_recv()

    def forward(l, k):
        return remote(kown.at[l, k], koth.at[l, k], f_s.at[l * 2 + k], f_r.at[l * 2 + k])

    to_mirror, to_next = 3 - 2 * (zl % 2), 1 + 2 * (zl % 2)
    full = [(to_mirror, 0), (to_mirror, 1), (2, 0), (2, 1), (to_next, 0), (to_next, 1), (0, 1)]

    load_first.wait()
    kv_send(0, 0, full[:3] + full[6:])

    load_suf.wait()
    load_len.wait()
    load_slot.wait()
    count = lengths[slot[0]]
    row = lax.broadcasted_iota(jnp.int32, (8, HD), 0)
    lane = lax.broadcasted_iota(jnp.int32, (8, HD), 1)
    valid = lane < count

    def suffix_head(h):
        cols = slice(h * HD, (h + 1) * HD)
        q = qmsg[h]
        s0 = dot(q, suf[0, 0, 0, :, cols], NT)
        s1 = dot(q, suf[1, 0, 0, :, cols], NT)
        s = jnp.where(valid, jnp.where(row < GROUP, s0, s1) * SCALE2, NEG)
        top = jnp.max(s, axis=1, keepdims=True)
        w = jnp.where(valid, jnp.exp2(s - top), 0.0).astype(bf16)
        den = jnp.sum(w.astype(f32), axis=1, keepdims=True)
        n0 = dot(w, suf[0, 0, 1, :, cols], NN)
        n1 = dot(w, suf[1, 0, 1, :, cols], NN)
        sbuf_o[h] = jnp.where(row < GROUP, n0, n1) / den
        sbuf_l[h] = jnp.broadcast_to(top + jnp.log2(den), (8, HD))

    def suffix_part():
        for h in range(KVH):
            suffix_head(h)

    suffix_part()

    def a_wait():
        remote(qa.at[0:7], qa.at[0:7], a_sem.at[0], a_sem.at[1]).wait_recv()

    a_wait()
    low = row < GROUP

    def regroup(a, b):
        return (jnp.where(low, a, pltpu.roll(b, GROUP, 0)), jnp.where(low, pltpu.roll(a, GROUP, 0), b))

    pairs = [regroup(qa[2 * j].astype(f32), qa[2 * j + 1].astype(f32)) for j in range(4)]
    qall[z, yl] = jnp.concatenate([p[l] for l in range(2) for p in pairs], axis=0).astype(bf16)
    mirror = zh * 4 + 3 - zl

    def b_send(block, z_to, r):
        remote(qall.at[block, yl], qall.at[block, yl], b_sem.at[0], r, at(head, yl, z_to, c)).start()

    def y_send(z_of):
        block = qall.at[z_of, yl]
        remote(block, block, y_sem.at[0], y_sem.at[1], at(head, 1 - yl, z, c)).start()

    b_send(z, mirror, b_sem.at[2])
    for k in (2, 1, 3):
        b_send(z, mate(k), b_sem.at[1])
    y_send(z)
    loads[1, 0].wait()
    kv_send(0, 0, full[3:6])
    kv_send(1, 0, full[:1])

    def m_wait():
        remote(qall.at[mirror, yl], qall.at[mirror, yl], b_sem.at[0], b_sem.at[2]).wait_recv()

    m_wait()
    for k in (2, 1, 3):
        b_send(mirror, mate(k), b_sem.at[3])
    y_send(mirror)
    loads[0, 1].wait()
    kv_send(1, 0, full[1:])
    kv_send(0, 1, full[:2])
    kv_wait(0, 0)
    forward(0, 0).start()

    def b_wait(r):
        remote(qall.at[0:3, 0], qall.at[0:3, 0], b_sem.at[0], b_sem.at[r]).wait_recv()

    def y_wait():
        whole = qall.at[:, 1 - yl]
        remote(whole, whole, y_sem.at[0], y_sem.at[1]).wait_recv()

    b_wait(1)
    for k in range(1, 4):
        y_send(mate(k))
    kv_send(0, 1, full[2:5])
    b_wait(3)
    for k in range(1, 4):
        y_send(mate(k) // 4 * 4 + 3 - mate(k) % 4)
    kv_send(0, 1, full[5:])
    loads[1, 1].wait()

    def weights(l):
        forward(l, 0).wait_recv()
        r64 = lax.broadcasted_iota(jnp.int32, (2, 64, HD), 1)
        c64 = lax.broadcasted_iota(jnp.int32, (2, 64, HD), 2)

        def rows(i, carry):
            q = qall[pl.ds(i * 2, 2), :, l * 32:(l + 1) * 32, :].reshape(128, HD)
            at_rows = pl.ds(pl.multiple_of(i * 128, 128), 128)
            sa = dot(q, kown[l, 0].reshape(HD, POS), NN) * SCALE2
            sb = dot(q, koth[l, 0].reshape(HD, POS), NN) * SCALE2
            top = jnp.maximum(jnp.max(sa, axis=1, keepdims=True), jnp.max(sb, axis=1, keepdims=True))
            wa = jnp.exp2(sa - top).astype(bf16)
            wb = jnp.exp2(sb - top).astype(bf16)
            den = jnp.sum(wa.astype(f32) + wb.astype(f32), axis=1, keepdims=True)
            wbuf[l, 0, at_rows, :] = wa
            wbuf[l, 1, at_rows, :] = wb
            rden[l, at_rows, :] = jnp.broadcast_to(1.0 / den, (128, HD))
            big = jnp.broadcast_to(top + jnp.log2(den), (128, HD)).reshape(2, 64, HD)
            line = jnp.sum(jnp.where(c64 == r64 + l * 64, big, 0.0), axis=1, keepdims=True)
            if l == 0:
                lsend[pl.ds(i * 2, 2)] = line
            else:
                lsend[pl.ds(i * 2, 2)] = lsend[pl.ds(i * 2, 2)] + line
            return carry

        lax.fori_loop(0, 4, rows, 0, unroll=True)

    z_at = [(z + d) % 8 for d in range(8)]
    x_at = [(x + d) % 4 for d in range(4)]
    y_at = [(y + d) % 4 for d in range(4)]

    def partials(l, offsets):
        for dz, dx, dy in offsets:
            z_to, x_to, y_to = z_at[dz], x_at[dx], y_at[dy]
            dev = ((x_to * 4 + y_to) * 4 + z_to % 4, z_to // 4 * 2 + c)
            remote(osend.at[l, z_to * 16 + y_to % 2 * 8 + x_to * 2 + y_to // 2],
                   orecv.at[l, spot * 8 + z], c_s.at[l], c_r.at[l], dev).start()

    def store_partials(l, o):
        osend.at[l].reshape(512, HD)[...] = o.astype(bf16)
        orecv[l, spot * 8 + z] = osend[l, z * 16 + yl * 8 + head]

    def values_own(l):
        oacc[l] = dot(wbuf[l, 0], kown[l, 1].reshape(HD, POS), NT)

    def values_other(l):
        forward(l, 1).wait_recv()
        store_partials(l, (oacc[l] + dot(wbuf[l, 1], koth[l, 1].reshape(HD, POS), NT)) * rden[l])

    def sources():
        ls = jnp.concatenate([lsend[...].reshape(8, HD), jnp.full((120, HD), NEG, f32)], axis=0).T
        for half in range(2):
            for j in range(4):
                base = half * 32 + j * 8
                even, odd = regroup(ls[base:base + 8], ls[64 + base:72 + base])
                gsend[4 * j + half] = even
                gsend[4 * j + 2 + half] = odd
        for k in range(1, 16):
            to = (spot + k) % 16
            remote(gsend.at[to], grecv.at[spot], g_sem.at[0], g_sem.at[1],
                   at(to // 2, to % 2, z, c)).start()
        grecv[spot] = gsend[spot]

    def columns():
        remote(grecv.at[0:15], grecv.at[0:15], g_sem.at[0], g_sem.at[1]).wait_recv()
        hsend[...] = grecv[...].reshape(128, HD).T[:8].reshape(8, 1, HD)
        for k in (4, 3, 5, 2, 6, 1, 7):
            to = (z + k) % 8
            remote(hsend.at[to], lrecv.at[z], l_sem.at[0], l_sem.at[1], at(head, yl, to, c)).start()
        lrecv[z] = hsend[z]

    kv_wait(1, 0)
    forward(1, 0).start()
    kv_send(1, 1, full, 0)
    y_wait()
    weights(0)
    kv_send(1, 1, full, 1)
    weights(1)
    sources()
    kv_wait(0, 1)
    forward(0, 1).start()
    values_own(0)

    first, second = slice(0, HALF), slice(HALF, POS)

    def last_first():
        owns[1, 1].wait()
        piece = kown.at[1, 1, 0:7, :, first]
        remote(piece, piece, kv_s.at[0], kv_r.at[3]).wait_recv()

    def last_copy():
        return remote(kown.at[1, 1, :, :, first], koth.at[1, 1, :, :, first], f_s.at[4], f_r.at[4])

    def last_dot(which, ref, span):
        return dot(wbuf[1, which, :, span], ref[1, 1, :, :, span].reshape(HD, HALF), NT)

    def values_first():
        oacc[1] = last_dot(0, kown, first)

    def last_pieces():
        own = kown.at[1, 1, part, :, second]
        remote(own, koth.at[1, 1, part, :, second], f_s.at[3], f_r.at[3]).start()
        for dz, dy in full:
            src = (yl + dy) % 2 * 4 + (zl + dz) % 4
            piece = kown.at[1, 1, src, :, second]
            remote(piece, piece, kv_s.at[0], v1_r.at[src]).wait_recv()
            remote(piece, koth.at[1, 1, src, :, second], f_s.at[3], f_r.at[3]).start()

    def values_second():
        oacc[1] = oacc[1] + last_dot(0, kown, second)
        last_copy().wait_recv()
        oacc[1] = oacc[1] + last_dot(1, koth, first)
        columns()
        whole = koth.at[1, 1, :, :, second]
        remote(whole, whole, f_s.at[3], f_r.at[3]).wait_recv()
        store_partials(1, (oacc[1] + last_dot(1, koth, second)) * rden[1])

    values_other(0)
    partials(0, FAR)
    last_first()
    last_copy().start()
    values_first()
    last_pieces()
    partials(0, NEAR)
    values_second()
    partials(1, FAR)
    partials(1, NEAR)

    def shares():
        remote(lrecv.at[0:7], lrecv.at[0:7], l_sem.at[0], l_sem.at[1]).wait_recv()
        ls = jnp.concatenate([lrecv[...].reshape(8, HD), jnp.full((120, HD), NEG, f32)], axis=0).T
        lfin[...] = ls.reshape(16, 8, HD)

        def one_head(h, carry):
            la, lb, lc = lfin[2 * h], lfin[2 * h + 1], sbuf_l[h]
            top = jnp.max(jnp.maximum(jnp.maximum(la, lb), lc), axis=1, keepdims=True)
            a, b, s = jnp.exp2(la - top), jnp.exp2(lb - top), jnp.exp2(lc - top)
            den = jnp.sum(a + b, axis=1, keepdims=True) + s
            sbuf_o[h] = s / den * sbuf_o[h]
            for half, w in enumerate((a / den, b / den)):
                for j in range(4):
                    pair = [jnp.broadcast_to(w[:, k:k + 1], (8, HD)) for k in (2 * j, 2 * j + 1)]
                    for l, tile in enumerate(regroup(*pair)):
                        share[l, 2 * h + half, j] = tile
            return carry

        lax.fori_loop(0, KVH, one_head, 0)

    def finish(l):
        remote(orecv.at[l, 0:127], orecv.at[l, 0:127], c_s.at[l], c_r.at[l]).wait_recv()
        got = orecv.at[l].reshape(512, HD)[...].astype(f32).reshape(KVH, 8, 8, HD)
        return jnp.sum(got * share[l].reshape(KVH, 8, 8, HD), axis=1)

    shares()
    o0 = finish(0)
    o1 = finish(1)
    for h in range(KVH):
        first_half, last_half = regroup(o0[h], o1[h])
        both = first_half + last_half + sbuf_o[h]
        for g in range(GROUP):
            pair = jnp.concatenate([both[g:g + 1], both[GROUP + g:GROUP + g + 1]], axis=0)
            out[:, (h * GROUP + g) * HD:(h * GROUP + g + 1) * HD] = pair.astype(bf16)

    remote(qa.at[0:7], qa.at[0:7], a_sem.at[0], a_sem.at[1]).wait_send()
    remote(qall.at[0:7, 0], qall.at[0:7, 0], b_sem.at[0], b_sem.at[1]).wait_send()
    remote(qall.at[:, yl], qall.at[:, yl], y_sem.at[0], y_sem.at[1]).wait_send()
    last_copy().wait_send()
    remote(kown.at[1, 1, :, :, second], koth.at[1, 1, :, :, second], f_s.at[3], f_r.at[3]).wait_send()
    remote(lrecv.at[0:7], lrecv.at[0:7], l_sem.at[0], l_sem.at[1]).wait_send()
    remote(grecv.at[0:15], grecv.at[0:15], g_sem.at[0], g_sem.at[1]).wait_send()
    for l in range(2):
        for k in range(2):
            remote(kown.at[l, k, 0:7], kown.at[l, k, 0:7], kv_s.at[l * 2 + k], kv_r.at[0]).wait_send()
            if (l, k) != (1, 1):
                forward(l, k).wait_send()
        remote(orecv.at[l, 0:127], orecv.at[l, 0:127], c_s.at[l], c_r.at[l]).wait_send()


def body(prefix_cache, queries, suffix_cache, suffix_lengths, slot_request):
    bf, f32 = jnp.bfloat16, jnp.float32
    dma = pltpu.SemaphoreType.DMA
    any_space = pl.BlockSpec(memory_space=pl.ANY)
    out = pl.pallas_call(
        kernel,
        out_shape=pltpu.VMEM((2, QH * HD), bf),
        in_specs=[
            any_space,
            any_space,
            any_space,
            any_space,
            any_space,
        ],
        out_specs=pl.BlockSpec(memory_space=pltpu.VMEM),
        scratch_shapes=[
            pltpu.SMEM((256,), jnp.int32),
            pltpu.SMEM((1,), jnp.int32),
            pltpu.VMEM((2, 2, 16, 8192), bf),
            pltpu.VMEM((2, 2, 8, 16, POS), bf),
            pltpu.VMEM((2, 2, 8, 16, POS), bf),
            pltpu.VMEM((2, 1, 2, SUF, KVH * HD), bf),
            pltpu.VMEM((2, QH * HD), bf),
            pltpu.VMEM((8, 8, HD), bf),
            pltpu.VMEM((8, 8, HD), bf),
            pltpu.VMEM((8, 2, 64, HD), bf),
            pltpu.VMEM((2, 2, 512, POS), bf),
            pltpu.VMEM((2, 512, HD), f32),
            pltpu.VMEM((2, 512, HD), f32),
            pltpu.VMEM((KVH, 8, HD), f32),
            pltpu.VMEM((KVH, 8, HD), f32),
            pltpu.VMEM((2, 128, GROUP, HD), bf),
            pltpu.VMEM((2, 128, GROUP, HD), bf),
            pltpu.VMEM((8, 1, HD), f32),
            pltpu.VMEM((8, 1, HD), f32),
            pltpu.VMEM((8, 1, HD), f32),
            pltpu.VMEM((16, 8, HD), f32),
            pltpu.VMEM((16, 8, HD), f32),
            pltpu.VMEM((16, 8, HD), f32),
            pltpu.VMEM((2, 16, 4, 8, HD), f32),
            dma((12,)),
            dma((2,)), dma((4,)), dma((2,)),
            dma((4,)), dma((4,)), dma((8,)),
            dma((5,)), dma((5,)),
            dma((2,)), dma((2,)),
            dma((2,)), dma((2,)),
        ],
        compiler_params=pltpu.CompilerParams(collective_id=0, has_side_effects=True),
        name="attend",
    )(prefix_cache, queries.reshape(2, QH * HD), suffix_cache, suffix_lengths, slot_request)
    return out.reshape(2, 1, QH * HD)


def solution(mesh):
    in_specs = (
        P(None, None, "seq", "rep"),
        P(None, ("seq", "rep"), None),
        P(None, ("seq", "rep"), None, None, None),
        P(),
        P(("seq", "rep")),
    )
    out_specs = P(None, ("seq", "rep"), None)
    return jax.shard_map(body, mesh=mesh, in_specs=in_specs, out_specs=out_specs, check_vma=False)
```

```python
import math

import jax
import jax.numpy as jnp
from jax import lax
from jax.experimental import pallas as pl
from jax.experimental.pallas import tpu as pltpu
from jax.sharding import PartitionSpec as P

QH = 32
KVH = 8
HD = 128
SUF = 128
GROUP = 4
NEG = -1e30
SCALE2 = HD ** -0.5 * math.log2(math.e)
POS = 1024
LAST = POS // 4
NT = (((1,), (1,)), ((), ()))
NN = (((1,), (0,)), ((), ()))
MESH = pl.DeviceIdType.MESH
OFFSETS = sorted(
    [(dz, dx, dy) for dz in range(8) for dx in range(4) for dy in range(4) if dz + dx + dy],
    key=lambda o: -(min(o[0], 8 - o[0]) + min(o[1], 4 - o[1]) + min(o[2], 4 - o[2])))
FAR, NEAR = OFFSETS[:64], OFFSETS[64:]


def dot(a, b, dims):
    return lax.dot_general(a, b, dims, preferred_element_type=jnp.float32)


def kernel(
    prefix, queries, suffix, lengths_in, slot_in, out,
    lengths, slot, stage, kown, koth, suf, qraw, qmsg, qa, qall, wbuf, rden, oacc, sbuf_o, sbuf_l,
    osend, orecv, lsend, hsend, lrecv, gsend, grecv, lfin, share,
    loc_sem, a_sem, b_sem, y_sem, kv_s, kv_r, v1_r, f_s, f_r, c_s, c_r, l_sem, g_sem,
):
    f32, bf16 = jnp.float32, jnp.bfloat16
    seq = lax.axis_index("seq")
    rep = lax.axis_index("rep")
    x, y, zl = seq // 16, (seq // 4) % 4, seq % 4
    yh, yl = y // 2, y % 2
    zh, c = rep // 2, rep % 2
    z = zh * 4 + zl
    head = x * 2 + yh
    part = yl * 4 + zl
    spot = head * 2 + yl

    def at(head_to, yl_to, z_to, c_to):
        x_to, yh_to = head_to // 2, head_to % 2
        return ((x_to * 4 + yh_to * 2 + yl_to) * 4 + z_to % 4, (z_to // 4) * 2 + c_to)

    other = at(head, yl, z, 1 - c)

    def remote(src, dst, s, r, dev=other):
        return pltpu.make_async_remote_copy(
            src_ref=src, dst_ref=dst, send_sem=s, recv_sem=r, device_id=dev, device_id_type=MESH)

    load_q = pltpu.make_async_copy(queries, qraw, loc_sem.at[9])
    load_first = pltpu.make_async_copy(prefix.at[0, 0], stage.at[0, 0], loc_sem.at[0])
    load_first.start()
    load_q.start()
    barrier = pltpu.get_barrier_semaphore()
    line = (z + 2) % 8

    def mate(k):
        return (line // 4 * 4 + (line + k) % 4 + 6) % 8

    peers = [other, at(head, 1 - yl, z, c)]
    for k in range(1, 8):
        peers.append(at((head + k) % 8, yl, z, c))
    for k in range(1, 4):
        peers.append(at(head, yl, zh * 4 + (zl + k) % 4, c))
        peers.append(at(head, 1 - yl, zh * 4 + (zl + k) % 4, c))
    for k in range(2):
        peers.append(at(head, yl, (line // 4 * 4 + (line % 4 // 2 * 2 + 2 + k) % 4 + 6) % 8, c))
    for dev in peers:
        pl.semaphore_signal(barrier, inc=1, device_id=dev, device_id_type=MESH)

    order = ((0, 0), (1, 0), (0, 1), (1, 1))
    loads = {(l, k): pltpu.make_async_copy(prefix.at[l, k], stage.at[l, k], loc_sem.at[l * 2 + k])
             for l, k in order[1:]}
    owns = {(l, k): pltpu.make_async_copy(
        prefix.at[l, k, :, pl.ds(pl.multiple_of(part * POS, POS), POS)],
        kown.at[l, k, part], loc_sem.at[4 + l * 2 + k]) for l, k in order}
    load_suf = pltpu.make_async_copy(suffix, suf, loc_sem.at[8])
    load_len = pltpu.make_async_copy(lengths_in, lengths, loc_sem.at[10])
    load_slot = pltpu.make_async_copy(slot_in, slot, loc_sem.at[11])
    load_suf.start()
    load_len.start()
    load_slot.start()

    for l, k in order:
        if (l, k) != (0, 0):
            loads[l, k].start()
        owns[l, k].start()

    load_q.wait()
    q32 = qraw[...].astype(f32)
    for h in range(KVH):
        rows = [q32[l:l + 1, (h * GROUP + g) * HD:(h * GROUP + g + 1) * HD]
                for l in range(2) for g in range(GROUP)]
        qmsg[h] = jnp.concatenate(rows, axis=0).astype(bf16)
    pl.semaphore_wait(barrier, len(peers))

    for k in range(1, 8):
        to = (head + k) % 8
        remote(qmsg.at[to], qa.at[head], a_sem.at[0], a_sem.at[1], at(to, yl, z, c)).start()
    qa[head] = qmsg[head]

    def kv_send(l, k, steps, half=None):
        for dz, dy in steps:
            yl_to, zl_to = (yl + dy) % 2, (zl + dz) % 4
            to = yl_to * 4 + zl_to
            if half is None:
                start, size, dst, r = 0, POS, kown.at[l, k, part], kv_r.at[l * 2 + k]
            else:
                start, size = (POS - LAST, LAST) if half else (0, POS - LAST)
                dst = kown.at[l, k, part, :, start:start + size]
                r = v1_r.at[part] if half else kv_r.at[l * 2 + k]
            remote(
                stage.at[l, k, :, pl.ds(pl.multiple_of(to * POS + start, LAST), size)],
                dst, kv_s.at[l * 2 + k], r, at(head, yl_to, zh * 4 + zl_to, c)).start()

    def kv_wait(l, k):
        owns[l, k].wait()
        remote(kown.at[l, k, 0:7], kown.at[l, k, 0:7], kv_s.at[0], kv_r.at[l * 2 + k]).wait_recv()

    def forward(l, k):
        return remote(kown.at[l, k], koth.at[l, k], f_s.at[l * 2 + k], f_r.at[l * 2 + k])

    to_mirror, to_next = 3 - 2 * (zl % 2), 1 + 2 * (zl % 2)
    full = [(to_mirror, 0), (to_mirror, 1), (2, 0), (2, 1), (to_next, 0), (to_next, 1), (0, 1)]

    load_first.wait()
    kv_send(0, 0, full[:3] + full[6:])

    load_suf.wait()
    load_len.wait()
    load_slot.wait()
    count = lengths[slot[0]]
    row = lax.broadcasted_iota(jnp.int32, (8, HD), 0)
    lane = lax.broadcasted_iota(jnp.int32, (8, HD), 1)
    valid = lane < count

    def suffix_head(h):
        cols = slice(h * HD, (h + 1) * HD)
        q = qmsg[h]
        s0 = dot(q, suf[0, 0, 0, :, cols], NT)
        s1 = dot(q, suf[1, 0, 0, :, cols], NT)
        s = jnp.where(valid, jnp.where(row < GROUP, s0, s1) * SCALE2, NEG)
        top = jnp.max(s, axis=1, keepdims=True)
        w = jnp.where(valid, jnp.exp2(s - top), 0.0).astype(bf16)
        den = jnp.sum(w.astype(f32), axis=1, keepdims=True)
        n0 = dot(w, suf[0, 0, 1, :, cols], NN)
        n1 = dot(w, suf[1, 0, 1, :, cols], NN)
        sbuf_o[h] = jnp.where(row < GROUP, n0, n1) / den
        sbuf_l[h] = jnp.broadcast_to(top + jnp.log2(den), (8, HD))

    def suffix_part():
        for h in range(KVH):
            suffix_head(h)

    suffix_part()

    def a_wait():
        remote(qa.at[0:7], qa.at[0:7], a_sem.at[0], a_sem.at[1]).wait_recv()

    a_wait()
    low = row < GROUP

    def regroup(a, b):
        return (jnp.where(low, a, pltpu.roll(b, GROUP, 0)), jnp.where(low, pltpu.roll(a, GROUP, 0), b))

    pairs = [regroup(qa[2 * j].astype(f32), qa[2 * j + 1].astype(f32)) for j in range(4)]
    qall[z, yl] = jnp.concatenate([p[l] for l in range(2) for p in pairs], axis=0).astype(bf16)
    mirror = zh * 4 + 3 - zl

    def b_send(block, z_to, r):
        remote(qall.at[block, yl], qall.at[block, yl], b_sem.at[0], r, at(head, yl, z_to, c)).start()

    def y_send(z_of):
        block = qall.at[z_of, yl]
        remote(block, block, y_sem.at[0], y_sem.at[1], at(head, 1 - yl, z, c)).start()

    b_send(z, mirror, b_sem.at[2])
    for k in (2, 1, 3):
        b_send(z, mate(k), b_sem.at[1])
    y_send(z)
    loads[1, 0].wait()
    kv_send(0, 0, full[3:6])
    kv_send(1, 0, full[:1])

    def m_wait():
        remote(qall.at[mirror, yl], qall.at[mirror, yl], b_sem.at[0], b_sem.at[2]).wait_recv()

    m_wait()
    for k in (2, 1, 3):
        b_send(mirror, mate(k), b_sem.at[3])
    y_send(mirror)
    loads[0, 1].wait()
    kv_send(1, 0, full[1:])
    kv_send(0, 1, full[:2])
    kv_wait(0, 0)
    forward(0, 0).start()

    def b_wait(r):
        remote(qall.at[0:3, 0], qall.at[0:3, 0], b_sem.at[0], b_sem.at[r]).wait_recv()

    def y_wait():
        whole = qall.at[:, 1 - yl]
        remote(whole, whole, y_sem.at[0], y_sem.at[1]).wait_recv()

    b_wait(1)
    for k in range(1, 4):
        y_send(mate(k))
    kv_send(0, 1, full[2:5])
    b_wait(3)
    for k in range(1, 4):
        y_send(mate(k) // 4 * 4 + 3 - mate(k) % 4)
    kv_send(0, 1, full[5:])
    loads[1, 1].wait()

    def weights(l):
        forward(l, 0).wait_recv()
        r64 = lax.broadcasted_iota(jnp.int32, (2, 64, HD), 1)
        c64 = lax.broadcasted_iota(jnp.int32, (2, 64, HD), 2)

        def rows(i, carry):
            q = qall[pl.ds(i * 2, 2), :, l * 32:(l + 1) * 32, :].reshape(128, HD)
            at_rows = pl.ds(pl.multiple_of(i * 128, 128), 128)
            sa = dot(q, kown[l, 0].reshape(HD, POS), NN) * SCALE2
            sb = dot(q, koth[l, 0].reshape(HD, POS), NN) * SCALE2
            top = jnp.maximum(jnp.max(sa, axis=1, keepdims=True), jnp.max(sb, axis=1, keepdims=True))
            wa = jnp.exp2(sa - top).astype(bf16)
            wb = jnp.exp2(sb - top).astype(bf16)
            den = jnp.sum(wa.astype(f32) + wb.astype(f32), axis=1, keepdims=True)
            wbuf[l, 0, at_rows, :] = wa
            wbuf[l, 1, at_rows, :] = wb
            rden[l, at_rows, :] = jnp.broadcast_to(1.0 / den, (128, HD))
            big = jnp.broadcast_to(top + jnp.log2(den), (128, HD)).reshape(2, 64, HD)
            line = jnp.sum(jnp.where(c64 == r64 + l * 64, big, 0.0), axis=1, keepdims=True)
            if l == 0:
                lsend[pl.ds(i * 2, 2)] = line
            else:
                lsend[pl.ds(i * 2, 2)] = lsend[pl.ds(i * 2, 2)] + line
            return carry

        lax.fori_loop(0, 4, rows, 0, unroll=True)

    z_at = [(z + d) % 8 for d in range(8)]
    x_at = [(x + d) % 4 for d in range(4)]
    y_at = [(y + d) % 4 for d in range(4)]

    def partials(l, offsets):
        for dz, dx, dy in offsets:
            z_to, x_to, y_to = z_at[dz], x_at[dx], y_at[dy]
            dev = ((x_to * 4 + y_to) * 4 + z_to % 4, z_to // 4 * 2 + c)
            remote(osend.at[l, z_to * 16 + y_to % 2 * 8 + x_to * 2 + y_to // 2],
                   orecv.at[l, spot * 8 + z], c_s.at[l], c_r.at[l], dev).start()

    def store_partials(l, o):
        osend.at[l].reshape(512, HD)[...] = o.astype(bf16)
        orecv[l, spot * 8 + z] = osend[l, z * 16 + yl * 8 + head]

    def values_own(l):
        oacc[l] = dot(wbuf[l, 0], kown[l, 1].reshape(HD, POS), NT)

    def values_other(l):
        forward(l, 1).wait_recv()
        store_partials(l, (oacc[l] + dot(wbuf[l, 1], koth[l, 1].reshape(HD, POS), NT)) * rden[l])

    def sources():
        ls = jnp.concatenate([lsend[...].reshape(8, HD), jnp.full((120, HD), NEG, f32)], axis=0).T
        for half in range(2):
            for j in range(4):
                base = half * 32 + j * 8
                even, odd = regroup(ls[base:base + 8], ls[64 + base:72 + base])
                gsend[4 * j + half] = even
                gsend[4 * j + 2 + half] = odd
        for k in range(1, 16):
            to = (spot + k) % 16
            remote(gsend.at[to], grecv.at[spot], g_sem.at[0], g_sem.at[1],
                   at(to // 2, to % 2, z, c)).start()
        grecv[spot] = gsend[spot]

    def columns():
        remote(grecv.at[0:15], grecv.at[0:15], g_sem.at[0], g_sem.at[1]).wait_recv()
        hsend[...] = grecv[...].reshape(128, HD).T[:8].reshape(8, 1, HD)
        for k in (4, 3, 5, 2, 6, 1, 7):
            to = (z + k) % 8
            remote(hsend.at[to], lrecv.at[z], l_sem.at[0], l_sem.at[1], at(head, yl, to, c)).start()
        lrecv[z] = hsend[z]

    kv_wait(1, 0)
    forward(1, 0).start()
    kv_send(1, 1, full, 0)
    y_wait()
    weights(0)
    kv_send(1, 1, full, 1)
    weights(1)
    sources()
    kv_wait(0, 1)
    forward(0, 1).start()
    values_own(0)

    first, second = slice(0, POS - LAST), slice(POS - LAST, POS)

    def last_first():
        owns[1, 1].wait()
        piece = kown.at[1, 1, 0:7, :, first]
        remote(piece, piece, kv_s.at[0], kv_r.at[3]).wait_recv()

    def last_copy():
        return remote(kown.at[1, 1, :, :, first], koth.at[1, 1, :, :, first], f_s.at[4], f_r.at[4])

    def last_dot(which, ref, span):
        return dot(wbuf[1, which, :, span], ref[1, 1, :, :, span].reshape(HD, span.stop - span.start), NT)

    def values_first():
        oacc[1] = last_dot(0, kown, first)

    def last_pieces():
        own = kown.at[1, 1, part, :, second]
        remote(own, koth.at[1, 1, part, :, second], f_s.at[3], f_r.at[3]).start()
        for dz, dy in full:
            src = (yl + dy) % 2 * 4 + (zl + dz) % 4
            piece = kown.at[1, 1, src, :, second]
            remote(piece, piece, kv_s.at[0], v1_r.at[src]).wait_recv()
            remote(piece, koth.at[1, 1, src, :, second], f_s.at[3], f_r.at[3]).start()

    def values_second():
        oacc[1] = oacc[1] + last_dot(0, kown, second)
        last_copy().wait_recv()
        oacc[1] = oacc[1] + last_dot(1, koth, first)
        columns()
        whole = koth.at[1, 1, :, :, second]
        remote(whole, whole, f_s.at[3], f_r.at[3]).wait_recv()
        store_partials(1, (oacc[1] + last_dot(1, koth, second)) * rden[1])

    values_other(0)
    partials(0, FAR)
    last_first()
    last_copy().start()
    values_first()
    last_pieces()
    values_second()
    partials(1, FAR)
    partials(1, NEAR)
    partials(0, NEAR)

    def shares():
        remote(lrecv.at[0:7], lrecv.at[0:7], l_sem.at[0], l_sem.at[1]).wait_recv()
        ls = jnp.concatenate([lrecv[...].reshape(8, HD), jnp.full((120, HD), NEG, f32)], axis=0).T
        lfin[...] = ls.reshape(16, 8, HD)

        def one_head(h, carry):
            la, lb, lc = lfin[2 * h], lfin[2 * h + 1], sbuf_l[h]
            top = jnp.max(jnp.maximum(jnp.maximum(la, lb), lc), axis=1, keepdims=True)
            a, b, s = jnp.exp2(la - top), jnp.exp2(lb - top), jnp.exp2(lc - top)
            den = jnp.sum(a + b, axis=1, keepdims=True) + s
            sbuf_o[h] = s / den * sbuf_o[h]
            for half, w in enumerate((a / den, b / den)):
                for j in range(4):
                    pair = [jnp.broadcast_to(w[:, k:k + 1], (8, HD)) for k in (2 * j, 2 * j + 1)]
                    for l, tile in enumerate(regroup(*pair)):
                        share[l, 2 * h + half, j] = tile
            return carry

        lax.fori_loop(0, KVH, one_head, 0)

    def finish(l):
        remote(orecv.at[l, 0:127], orecv.at[l, 0:127], c_s.at[l], c_r.at[l]).wait_recv()
        got = orecv.at[l].reshape(512, HD)[...].astype(f32).reshape(KVH, 8, 8, HD)
        return jnp.sum(got * share[l].reshape(KVH, 8, 8, HD), axis=1)

    shares()
    o0 = finish(0)
    o1 = finish(1)
    for h in range(KVH):
        first_half, last_half = regroup(o0[h], o1[h])
        both = first_half + last_half + sbuf_o[h]
        for g in range(GROUP):
            pair = jnp.concatenate([both[g:g + 1], both[GROUP + g:GROUP + g + 1]], axis=0)
            out[:, (h * GROUP + g) * HD:(h * GROUP + g + 1) * HD] = pair.astype(bf16)

    remote(qa.at[0:7], qa.at[0:7], a_sem.at[0], a_sem.at[1]).wait_send()
    remote(qall.at[0:7, 0], qall.at[0:7, 0], b_sem.at[0], b_sem.at[1]).wait_send()
    remote(qall.at[:, yl], qall.at[:, yl], y_sem.at[0], y_sem.at[1]).wait_send()
    last_copy().wait_send()
    remote(kown.at[1, 1, :, :, second], koth.at[1, 1, :, :, second], f_s.at[3], f_r.at[3]).wait_send()
    remote(lrecv.at[0:7], lrecv.at[0:7], l_sem.at[0], l_sem.at[1]).wait_send()
    remote(grecv.at[0:15], grecv.at[0:15], g_sem.at[0], g_sem.at[1]).wait_send()
    for l in range(2):
        for k in range(2):
            remote(kown.at[l, k, 0:7], kown.at[l, k, 0:7], kv_s.at[l * 2 + k], kv_r.at[0]).wait_send()
            if (l, k) != (1, 1):
                forward(l, k).wait_send()
        remote(orecv.at[l, 0:127], orecv.at[l, 0:127], c_s.at[l], c_r.at[l]).wait_send()


def body(prefix_cache, queries, suffix_cache, suffix_lengths, slot_request):
    bf, f32 = jnp.bfloat16, jnp.float32
    dma = pltpu.SemaphoreType.DMA
    any_space = pl.BlockSpec(memory_space=pl.ANY)
    out = pl.pallas_call(
        kernel,
        out_shape=pltpu.VMEM((2, QH * HD), bf),
        in_specs=[
            any_space,
            any_space,
            any_space,
            any_space,
            any_space,
        ],
        out_specs=pl.BlockSpec(memory_space=pltpu.VMEM),
        scratch_shapes=[
            pltpu.SMEM((256,), jnp.int32),
            pltpu.SMEM((1,), jnp.int32),
            pltpu.VMEM((2, 2, 16, 8192), bf),
            pltpu.VMEM((2, 2, 8, 16, POS), bf),
            pltpu.VMEM((2, 2, 8, 16, POS), bf),
            pltpu.VMEM((2, 1, 2, SUF, KVH * HD), bf),
            pltpu.VMEM((2, QH * HD), bf),
            pltpu.VMEM((8, 8, HD), bf),
            pltpu.VMEM((8, 8, HD), bf),
            pltpu.VMEM((8, 2, 64, HD), bf),
            pltpu.VMEM((2, 2, 512, POS), bf),
            pltpu.VMEM((2, 512, HD), f32),
            pltpu.VMEM((2, 512, HD), f32),
            pltpu.VMEM((KVH, 8, HD), f32),
            pltpu.VMEM((KVH, 8, HD), f32),
            pltpu.VMEM((2, 128, GROUP, HD), bf),
            pltpu.VMEM((2, 128, GROUP, HD), bf),
            pltpu.VMEM((8, 1, HD), f32),
            pltpu.VMEM((8, 1, HD), f32),
            pltpu.VMEM((8, 1, HD), f32),
            pltpu.VMEM((16, 8, HD), f32),
            pltpu.VMEM((16, 8, HD), f32),
            pltpu.VMEM((16, 8, HD), f32),
            pltpu.VMEM((2, 16, 4, 8, HD), f32),
            dma((12,)),
            dma((2,)), dma((4,)), dma((2,)),
            dma((4,)), dma((4,)), dma((8,)),
            dma((5,)), dma((5,)),
            dma((2,)), dma((2,)),
            dma((2,)), dma((2,)),
        ],
        compiler_params=pltpu.CompilerParams(collective_id=0, has_side_effects=True),
        name="attend",
    )(prefix_cache, queries.reshape(2, QH * HD), suffix_cache, suffix_lengths, slot_request)
    return out.reshape(2, 1, QH * HD)


def solution(mesh):
    in_specs = (
        P(None, None, "seq", "rep"),
        P(None, ("seq", "rep"), None),
        P(None, ("seq", "rep"), None, None, None),
        P(),
        P(("seq", "rep")),
    )
    out_specs = P(None, ("seq", "rep"), None)
    return jax.shard_map(body, mesh=mesh, in_specs=in_specs, out_specs=out_specs, check_vma=False)
```
